32 devices in a mesh: gx: 4 (over z), gy: 2 (over y), gz: 4 (over x, core).
Axes of the slice: x: 2, y: 2, z: 4, core: 2. Of those that a mesh axis runs over, the one named last changes fastest.
Arguments:
- colloc: bfloat16 [768, 4000], P(('gx', 'gy')), may hold values from -6 to 6
- occ_coeffs: bfloat16 [4000, 1024], P(None, 'gz'), may hold values from -0.09375 to 0.09375
- core: bfloat16 [768, 2, 384], P('gx', 'gy'), may hold values from -6.246567e-05 to 6.246567e-05
Outputs:
- coulomb: float32 [96, 4000], P(('gx', 'gz'), 'gy')
- exchange: float32 [96, 4000], P(('gx', 'gz'), 'gy')
The draws below stay inside these ranges and needn't reach their ends.
All inputs are finite; a program needn't handle non-finite values.
Results may differ from the reference program's by a relative error of at most 0.0089.
Values may be sent and summed in bfloat16 or wider, within the bound.
A program may use at most 64 MiB of HBM per device.

```python
import jax
import jax.numpy as jnp
from jax import lax

N = 4000
O = 1024
PB = 96
W = 96
P_SIZE = 768
N_GX = 4
N_GY = 2
N_GZ = 4


def block_levels(rng, extent, cuts, least, top_value):
    def one(position, blocks):
        heights = jax.random.uniform(jax.random.fold_in(jax.random.fold_in(rng, 6), position), (blocks,), jnp.float32, least / len(cuts), top_value / len(cuts))
        return jnp.repeat(jnp.exp(heights), extent[position] // blocks).reshape((-1,) + (1,) * (len(extent) - position - 1))

    loudness = one(*cuts[0])
    for cut in cuts[1:]:
        loudness = loudness * one(*cut)
    return loudness


def scatter_about(stream_key, extent, deviation, reach, pieces=(), kind=jnp.bfloat16):
    values = deviation * jax.random.normal(stream_key, extent, jnp.float32)
    if pieces:
        values = values * block_levels(stream_key, extent, pieces, -0.22, 0.18)
    return jnp.clip(values, -reach, reach).astype(kind)


def setup_inputs(seed: int = 0) -> dict:
    splits = jax.random.split(jax.random.key(seed), 4)
    colloc = scatter_about(splits[0], (P_SIZE, N), 1.0, 6.0, ((0, 8),))
    occ_coeffs = scatter_about(splits[1], (N, O), N ** -0.5, 0.09375, ((1, 4),))
    core = scatter_about(splits[2], (P_SIZE, N_GY, N_GX * PB), (0.008 / (PB * N_GX * N_GY)), 6.246566772460938e-05, ((0, 4), (1, 2)))
    return dict(colloc=colloc, occ_coeffs=occ_coeffs, core=core)


def reference(colloc, occ_coeffs, core):
    zmat = core.reshape(P_SIZE, N_GY, N_GX, PB).transpose(0, 2, 1, 3).reshape(P_SIZE, P_SIZE)
    occ = jnp.dot(colloc, occ_coeffs, preferred_element_type=jnp.float32).astype(jnp.bfloat16)
    density = jnp.sum(jnp.square(occ.astype(jnp.float32)), axis=1).astype(jnp.bfloat16)
    potential = jnp.dot(zmat, density, preferred_element_type=jnp.float32)
    window = colloc[:, :W]
    block_rows = PB * N_GY
    quarter = O // N_GZ

    def add_block(index, acc):
        start = (index * block_rows).astype(jnp.int32)
        occ_rows = lax.dynamic_slice_in_dim(occ, start, block_rows, 0)
        core_rows = lax.dynamic_slice_in_dim(zmat, start, block_rows, 0)
        win_rows = lax.dynamic_slice_in_dim(window, start, block_rows, 0)
        for group in range(N_GZ):
            left = occ_rows[:, group * quarter:(group + 1) * quarter]
            right = occ[:, group * quarter:(group + 1) * quarter]
            gram = jnp.dot(left, right.T, preferred_element_type=jnp.float32)
            mixed = (core_rows.astype(jnp.float32) * gram).astype(jnp.bfloat16)
            acc = acc + jnp.dot(mixed.T, win_rows, preferred_element_type=jnp.float32)
        return acc

    totals = lax.fori_loop(0, N_GX, add_block, jnp.zeros((P_SIZE, W), jnp.float32))
    weighted = (window.astype(jnp.float32) * potential[:, None]).astype(jnp.bfloat16)
    coulomb = jnp.dot(weighted.T, colloc, preferred_element_type=jnp.float32)
    exchange = jnp.dot(totals.astype(jnp.bfloat16).T, colloc, preferred_element_type=jnp.float32)
    return (coulomb, exchange)
```

```python
import functools

import jax
import jax.numpy as jnp
import numpy as np
from jax import lax
from jax.experimental import pallas as pl
from jax.experimental.pallas import tpu as pltpu
from jax.sharding import PartitionSpec as P

W = 96
LANES = 128
DEPTH = 1024
MESH = pl.DeviceIdType.MESH
F32 = jnp.float32
BF16 = jnp.bfloat16


def up(value, step):
    return -(-value // step) * step


def dot(left, right, left_dim, right_dim):
    return lax.dot_general(
        left, right, (((left_dim,), (right_dim,)), ((), ())), preferred_element_type=F32
    )


def kernel(
    dims,
    colloc_hbm,
    coeffs_hbm,
    core_hbm,
    place_hbm,
    out_ref,
    vals,
    coeffs,
    core,
    place,
    cores,
    core_t,
    row_occ,
    col_occ,
    row_win,
    col_win,
    win_t,
    dens,
    stage,
    cols,
    pot_send,
    pot_recv,
    tot_send,
    tot_recv,
    z_send,
    z_recv,
    load_sem,
    depth_sem,
    ready,
    core_sem,
    core_fwd_sem,
    row_sem,
    col_sem,
    row_win_sem,
    row_win_fwd_sem,
    col_win_sem,
    dens_sem,
    cols_sem,
    cols_fwd_sem,
    pot_sem,
    tot_sem,
    z_sem,
):
    gx_size, gy_size, gz_size, rows, width = dims
    gx, gy, gz = lax.axis_index("gx"), lax.axis_index("gy"), lax.axis_index("gz")
    points, total = vals.shape
    lanes = row_win.shape[3]
    halves, half = row_win.shape[1], row_win.shape[2]
    span = cols.shape[2]
    side = gy_size * points
    part = lax.rem(gz, halves)

    def turn(pos, step, size):
        if size & (size - 1):
            return lax.rem(pos + step, size) if step else pos
        bit = 1
        while bit <= step:
            if step & bit:
                pos = pos + bit * (1 - 2 * lax.rem(lax.div(pos, bit), 2))
            bit *= 2
        return pos

    planes = [turn(gx, d, gx_size) for d in range(1, gx_size)]
    sides = [turn(gy, d, gy_size) for d in range(1, gy_size)]
    flat = [
        (turn(gy, dy, gy_size), turn(gz, dz, gz_size))
        for dy in range(gy_size)
        for dz in range(gz_size)
        if dy or dz
    ]
    mate = (gx, gy, turn(gz, 1, gz_size))

    def copy(src, dst, sems, out_slot, in_slot, target):
        return pltpu.make_async_remote_copy(
            src_ref=src,
            dst_ref=dst,
            send_sem=sems.at[(0,) + out_slot],
            recv_sem=sems.at[(1,) + in_slot],
            device_id=target,
            device_id_type=MESH,
        )

    def arrive(dst, sems, in_slot):
        copy(dst, dst, sems, in_slot, in_slot, mate).wait_recv()

    def core_copy(t, h):
        whole = cores.at[t, h], core_t.at[gx, :, gy]
        return copy(*whole, core_sem, (t, h), (gx, gy), (t, h, gz))

    def core_part_copy(t, h):
        some = cores.at[t, h, part], core_t.at[gx, part, gy]
        return copy(*some, core_sem, (t, h), (gx, gy), (t, h, gz))

    def core_fwd(z):
        some = core_t.at[z, part]
        return copy(some, some, core_fwd_sem, (z,), (z,), mate)

    def row_win_copy(t):
        src = vals.at[pl.ds(pl.multiple_of(part * half, half), half), pl.ds(0, lanes)]
        return copy(src, row_win.at[gx, part], row_win_sem, (t,), (gx,), (t, gy, gz))

    def row_win_fwd(z):
        some = row_win.at[z, part]
        return copy(some, some, row_win_fwd_sem, (z,), (z,), mate)

    def col_win_copy(h):
        src = vals.at[:, pl.ds(0, lanes)]
        return copy(src, col_win.at[gy], col_win_sem, (h,), (gy,), (gx, h, gz))

    def dens_copy(t):
        some = dens.at[gx]
        return copy(some, some, dens_sem, (t,), (gx,), (t, gy, gz))

    def row_copy(t):
        some = row_occ.at[gx]
        return copy(some, some, row_sem, (t,), (gx,), (t, gy, gz))

    def col_copy(h):
        some = col_occ.at[gy]
        return copy(some, some, col_sem, (h,), (gy,), (gx, h, gz))

    def cols_copy(h):
        at = pl.ds(pl.multiple_of(part * half, half), half)
        return copy(stage.at[h, at], cols.at[gy, at], cols_sem, (h,), (gy,), (gx, h, gz))

    def cols_fwd(h):
        some = cols.at[h, pl.ds(pl.multiple_of(part * half, half), half)]
        return copy(some, some, cols_fwd_sem, (h,), (h,), mate)

    mine = gy * gz_size + gz

    def pot_copy(h, g):
        return copy(pot_send, pot_recv.at[mine], pot_sem, (h * gz_size + g,), (mine,), (gx, h, g))

    def tot_copy(h, g):
        slots = (h * gz_size + g,), (mine,)
        return copy(tot_send.at[g], tot_recv.at[mine], tot_sem, *slots, (gx, h, g))

    def z_copy(index, t):
        dst = z_recv.at[index, gx]
        return copy(z_send.at[index, t], dst, z_sem, (index, t), (index, gx), (t, gy, gz))

    load_core = pltpu.make_async_copy(core_hbm, core, load_sem.at[0])
    load_vals = pltpu.make_async_copy(colloc_hbm, vals, load_sem.at[1])
    load_place = pltpu.make_async_copy(place_hbm, place, load_sem.at[2])
    spans = [(s, min(DEPTH, total - s)) for s in range(0, total, DEPTH)]
    depth_loads = [
        pltpu.make_async_copy(
            coeffs_hbm.at[pl.ds(s, n)], coeffs.at[pl.ds(s, n)], depth_sem.at[i]
        )
        for i, (s, n) in enumerate(spans)
    ]
    load_core.start()
    load_vals.start()
    for load in depth_loads:
        load.start()
    load_place.start()

    barrier = pltpu.get_barrier_semaphore()
    for h, g in flat:
        pl.semaphore_signal(barrier, inc=1, device_id=(gx, h, g), device_id_type=MESH)
    for t in range(1, gx_size):

        @pl.when(gx < t)
        def _():
            for h in range(gy_size):
                pl.semaphore_signal(barrier, inc=1, device_id=(t, h, gz), device_id_type=MESH)

    load_core.wait()
    for a in range(gx_size):
        block = core[:, a * points : (a + 1) * points]
        cores[a] = block.reshape(cores.shape[1:])

    pl.semaphore_wait(barrier, len(flat) + gx * gy_size)
    for t in range(gx_size - 1):

        @pl.when(gx > t)
        def _():
            for h in range(gy_size):
                pl.semaphore_signal(
                    ready.at[gx], inc=1, device_id=(t, h, gz), device_id_type=MESH
                )
            for h in range(gy_size):
                core_part_copy(t, h).start()

    for h in sides:
        core_copy(gx, h).start()
    core_t[gx, :, gy] = cores[gx, gy]

    load_vals.wait()
    for t in range(gx_size - 1):

        @pl.when(gx > t)
        def _():
            row_win_copy(t).start()

    for h in sides:
        col_win_copy(h).start()
    for h in range(gy_size):
        stage[h, :, :width] = vals[:, h * width : (h + 1) * width]
        if width < span:
            stage[h, :, width:] = jnp.zeros((points, span - width), BF16)
    own_cols = pltpu.make_async_copy(stage.at[gy], cols.at[gy], load_sem.at[3])

    occ = jnp.zeros((points, coeffs.shape[1]), F32)
    for i, (s, n) in enumerate(spans):
        depth_loads[i].wait()
        occ += dot(vals[:, s : s + n], coeffs[s : s + n, :], 1, 0)
    occ = occ.astype(BF16)
    row_occ[gx] = occ
    col_occ[gy] = occ
    square = jnp.square(occ.astype(F32))
    high = square.astype(BF16)
    low = (square - high.astype(F32)).astype(BF16)
    ones = jnp.ones((8, occ.shape[1]), BF16)
    dens[gx] = dot(ones, high, 1, 1) + dot(ones, low, 1, 1)
    for t in range(gx_size - 1):

        @pl.when(gx > t)
        def _():
            dens_copy(t).start()
            row_copy(t).start()

    for h in sides:
        col_copy(h).start()
    for h in sides:
        cols_copy(h).start()
    own_cols.start()
    for t in range(1, gx_size):

        @pl.when(gx < t)
        def _():
            pl.semaphore_wait(ready.at[t], gy_size)
            for h in range(gy_size):
                core_part_copy(t, h).start()
            dens_copy(t).start()
            row_win_copy(t).start()
            row_copy(t).start()

    own_win = vals[:, :lanes]
    row_win[gx] = own_win.reshape(row_win.shape[1:])
    col_win[gy] = own_win
    load_place.wait()
    spread = place[...]

    for z in planes:
        for h in range(gy_size):
            arrive(core_t.at[z, part, h], core_sem, (z, h))
        if halves > 1:
            core_fwd(z).start()
        arrive(row_win.at[z, part], row_win_sem, (z,))
        if halves > 1:
            row_win_fwd(z).start()

    def potential_of(z):
        return dot(dens[z].astype(BF16), cores[z].reshape(side, points), 1, 1)

    potential = potential_of(gx)
    for z in planes:
        arrive(dens.at[z], dens_sem, (z,))
        potential += potential_of(z)
    pot_send[...] = potential
    for h, g in flat:
        pot_copy(h, g).start()

    for h in sides:
        arrive(core_t.at[gx, :, h], core_sem, (gx, h))
        arrive(col_win.at[h], col_win_sem, (h,))
        arrive(col_occ.at[h], col_sem, (h,))
    win_t[...] = dot(spread, col_win[...].reshape(side, lanes), 0, 1).reshape(win_t.shape)
    col_vals = col_occ[...].reshape(side, col_occ.shape[2])

    block = None
    for i, z in enumerate([gx] + planes):
        if i:
            if halves > 1:
                other = 1 - part
                arrive(core_t.at[z, other], core_fwd_sem, (z,))
                arrive(row_win.at[z, other], row_win_fwd_sem, (z,))
            arrive(row_occ.at[z], row_sem, (z,))
        win_rows = dot(spread, row_win[z].reshape(points, lanes), 0, 1).astype(BF16)
        gram = dot(row_occ[z], col_vals, 1, 1)
        core_vals = jnp.concatenate(
            [core_t[z, :, h].reshape(points, points) for h in range(gy_size)], axis=1
        )
        mixed = (core_vals.astype(F32) * gram).astype(BF16)
        term = dot(win_rows, mixed, 1, 0)
        block = term if block is None else block + term
    tot_send[...] = block.reshape(tot_send.shape).astype(BF16)
    for h, g in flat:
        tot_copy(h, g).start()

    for h in sides:
        at = pl.ds(pl.multiple_of(part * half, half), half)
        arrive(cols.at[h, at], cols_sem, (h,))
        if halves > 1:
            cols_fwd(h).start()

    def spread_out(index, left):
        spare = jnp.zeros((8 - rows, side), F32)
        lines = []
        for a in range(gx_size):
            lines += [left[a * rows : (a + 1) * rows], spare]
        lefts = jnp.concatenate(lines, axis=0).astype(BF16)
        out = dot(lefts, cols[...].reshape(side, span), 1, 0)
        z_send[index] = out.reshape(gx_size, 8, span).astype(BF16)
        for t in planes[::-1]:
            z_copy(index, t).start()

    pot = pot_send[...]
    for h, g in flat:
        slot = h * gz_size + g
        arrive(pot_recv.at[slot], pot_sem, (slot,))
        pot += pot_recv[slot]
    weighted = (win_t[gz] * pot[:1]).astype(BF16).astype(F32)
    own_cols.wait()
    if halves > 1:
        for h in sides:
            at = pl.ds(pl.multiple_of((1 - part) * half, half), half)
            arrive(cols.at[h, at], cols_fwd_sem, (h,))
    spread_out(0, weighted)

    owned = tot_send[gz].astype(F32)
    for h, g in flat:
        slot = h * gz_size + g
        arrive(tot_recv.at[slot], tot_sem, (slot,))
        owned += tot_recv[slot].astype(F32)
    tight = win_t.shape[1]
    owned = owned.reshape(-1, side)[:tight]
    spread_out(1, owned)

    for index in range(2):
        acc = z_send[index, gx].astype(F32)
        for z in planes:
            arrive(z_recv.at[index, z], z_sem, (index, z))
            acc += z_recv[index, z].astype(F32)
        out_ref[index] = acc[:rows, :width]

    for h in sides:
        core_copy(gx, h).wait_send()
        col_win_copy(h).wait_send()
        col_copy(h).wait_send()
        cols_copy(h).wait_send()
        if halves > 1:
            cols_fwd(h).wait_send()
    for t in planes:
        for h in range(gy_size):
            core_part_copy(t, h).wait_send()
        row_win_copy(t).wait_send()
        dens_copy(t).wait_send()
        row_copy(t).wait_send()
        if halves > 1:
            core_fwd(t).wait_send()
            row_win_fwd(t).wait_send()
        for index in range(2):
            z_copy(index, t).wait_send()
    for h, g in flat:
        pot_copy(h, g).wait_send()
        tot_copy(h, g).wait_send()


def local(colloc, occ_coeffs, core):
    points, total = colloc.shape
    gx_size = lax.axis_size("gx")
    gy_size = lax.axis_size("gy")
    gz_size = lax.axis_size("gz")
    occupied = occ_coeffs.shape[1]
    rows = W // (gx_size * gz_size)
    width = total // gy_size
    row_count, flat = core.shape[0], core.shape[2]
    lanes = up(W, LANES)
    side = gy_size * points
    span = up(width, LANES)
    halves = 2 if gz_size % 2 == 0 else 1
    half = points // halves

    used = gx_size * rows
    tight = up(used, 8)
    place = np.zeros((lanes, gz_size, tight), np.float32)
    for a in range(gx_size):
        for g in range(gz_size):
            for k in range(rows):
                place[(a * gz_size + g) * rows + k, g, a * rows + k] = 1
    place = jnp.asarray(place.reshape(lanes, gz_size * tight), BF16)

    dims = (gx_size, gy_size, gz_size, rows, width)
    dma = pltpu.SemaphoreType.DMA
    vmem = pltpu.VMEM
    result = pl.pallas_call(
        functools.partial(kernel, dims),
        out_shape=pltpu.VMEM((2, rows, width), F32),
        in_specs=[pl.BlockSpec(memory_space=pltpu.HBM)] * 4,
        out_specs=pl.BlockSpec(memory_space=pltpu.VMEM),
        scratch_shapes=[
            vmem((points, total), BF16),
            vmem((total, occupied), BF16),
            vmem((row_count, flat), BF16),
            vmem(place.shape, BF16),
            vmem((gx_size, gy_size, halves, half, points), BF16),
            vmem((gx_size, halves, gy_size, half, points), BF16),
            vmem((gx_size, points, occupied), BF16),
            vmem((gy_size, points, occupied), BF16),
            vmem((gx_size, halves, half, lanes), BF16),
            vmem((gy_size, points, lanes), BF16),
            vmem((gz_size, tight, side), F32),
            vmem((gx_size, 8, points), F32),
            vmem((gy_size, points, span), BF16),
            vmem((gy_size, points, span), BF16),
            vmem((8, side), F32),
            vmem((gy_size * gz_size, 8, side), F32),
            vmem((gz_size, tight // 8, 8, side), BF16),
            vmem((gy_size * gz_size, tight // 8, 8, side), BF16),
            vmem((2, gx_size, 8, span), BF16),
            vmem((2, gx_size, 8, span), BF16),
            dma((4,)),
            dma((-(-total // DEPTH),)),
            pltpu.SemaphoreType.REGULAR((gx_size,)),
            dma((2, gx_size, gy_size)),
            dma((2, gx_size)),
            dma((2, gx_size)),
            dma((2, gy_size)),
            dma((2, gx_size)),
            dma((2, gx_size)),
            dma((2, gy_size)),
            dma((2, gx_size)),
            dma((2, gy_size)),
            dma((2, gy_size)),
            dma((2, gy_size * gz_size)),
            dma((2, gy_size * gz_size)),
            dma((2, 2, gx_size)),
        ],
        compiler_params=pltpu.CompilerParams(
            collective_id=0, has_side_effects=True, vmem_limit_bytes=60 * 1024 * 1024
        ),
    )(colloc, occ_coeffs, core.reshape(row_count, flat), place)
    return result[0], result[1]


def solution(mesh):
    in_specs = (P(("gx", "gy"), None), P(None, "gz"), P("gx", "gy", None))
    out_specs = (P(("gx", "gz"), "gy"), P(("gx", "gz"), "gy"))
    return jax.shard_map(local, mesh=mesh, in_specs=in_specs, out_specs=out_specs, check_vma=False)
```

```python
import functools

import jax
import jax.numpy as jnp
import numpy as np
from jax import lax
from jax.experimental import pallas as pl
from jax.experimental.pallas import tpu as pltpu
from jax.sharding import PartitionSpec as P

W = 96
LANES = 128
DEPTH = 1024
MESH = pl.DeviceIdType.MESH
F32 = jnp.float32
BF16 = jnp.bfloat16


def up(value, step):
    return -(-value // step) * step


def dot(left, right, left_dim, right_dim):
    return lax.dot_general(
        left, right, (((left_dim,), (right_dim,)), ((), ())), preferred_element_type=F32
    )


def kernel(
    dims,
    colloc_hbm,
    coeffs_hbm,
    core_hbm,
    place_hbm,
    out_ref,
    vals,
    coeffs,
    core,
    place,
    core_q,
    row_occ,
    col_occ,
    col_win,
    win_t,
    dens,
    stage,
    cols,
    pot_send,
    pot_recv,
    tot_send,
    tot_recv,
    z_send,
    z_recv,
    load_sem,
    depth_sem,
    ready,
    known,
    row_sem,
    col_sem,
    col_win_sem,
    dens_sem,
    cols_sem,
    pot_sem,
    tot_sem,
    z_sem,
):
    gx_size, gy_size, gz_size, rows, width = dims
    gx, gy, gz = lax.axis_index("gx"), lax.axis_index("gy"), lax.axis_index("gz")
    points, total = vals.shape
    lanes = col_win.shape[2]
    crowd = gy_size * gz_size
    halves = 2 if gz_size % 2 == 0 else 1
    half = points // halves
    base = gz - lax.rem(gz, halves)
    span = cols.shape[2]
    side = gy_size * points
    part = lax.rem(gz, halves)

    def turn(pos, step, size):
        if size & (size - 1):
            return lax.rem(pos + step, size) if step else pos
        bit = 1
        while bit <= step:
            if step & bit:
                pos = pos + bit * (1 - 2 * lax.rem(lax.div(pos, bit), 2))
            bit *= 2
        return pos

    planes = [turn(gx, d, gx_size) for d in range(1, gx_size)]
    sides = [turn(gy, d, gy_size) for d in range(1, gy_size)]
    flat = [
        (turn(gy, dy, gy_size), turn(gz, dz, gz_size))
        for dy in range(gy_size)
        for dz in range(gz_size)
        if dy or dz
    ]
    mine = gy * gz_size + gz
    own = gy * halves + part
    mate = (gx, gy, turn(gz, 1, gz_size))

    def copy(src, dst, sems, target, slot=0):
        return pltpu.make_async_remote_copy(
            src_ref=src,
            dst_ref=dst,
            send_sem=sems.at[0],
            recv_sem=sems.at[1 + slot],
            device_id=target,
            device_id_type=MESH,
        )

    def arrive(ref, sems, slot=0):
        copy(ref, ref, sems, mate, slot).wait_recv()

    def leave(ref, sems):
        copy(ref, ref, sems, mate).wait_send()

    def seat(i):
        return lax.div(i, gz_size), lax.rem(i, gz_size)

    def sweep(body):
        if crowd <= 16:
            for i in range(crowd):
                body(jnp.int32(i))
        else:
            lax.fori_loop(0, crowd, lambda i, c: (body(i), c)[1], 0)

    own_rows = pl.ds(pl.multiple_of(part * half, half), half)

    def col_win_copy(h):
        return copy(vals.at[:, pl.ds(0, lanes)], col_win.at[gy], col_win_sem, (gx, h, gz))

    def dens_copy(t):
        some = dens.at[gx]
        return copy(some, some, dens_sem, (t, gy, gz))

    def row_copy(t, k):
        src = col_occ.at[own, pl.ds(k * half, half)]
        return copy(src, row_occ.at[gx * halves + part], row_sem, (t, gy, base + k), gx)

    def col_copy(h):
        some = col_occ.at[own]
        return copy(some, some, col_sem, (gx, h, gz))

    def col_fwd(h):
        some = col_occ.at[h * halves + part]
        return copy(some, some, col_sem, mate, 1)

    def cols_copy(h):
        at = pl.ds(pl.multiple_of(part * half, half), half)
        return copy(stage.at[h, at], cols.at[gy, at], cols_sem, (gx, h, gz))

    def cols_fwd(h):
        some = cols.at[h, pl.ds(pl.multiple_of(part * half, half), half)]
        return copy(some, some, cols_sem, mate, 1)

    def pot_copy(h, g):
        return copy(pot_send, pot_recv.at[mine], pot_sem, (gx, h, g))

    def tot_copy(t, h, g):
        return copy(tot_send.at[t, g], tot_recv.at[gx * crowd + mine], tot_sem, (t, h, g))

    def z_copy(index, t):
        return copy(z_send.at[index, t], z_recv.at[index, gx], z_sem, (t, gy, gz), index)

    load_core = pltpu.make_async_copy(core_hbm, core, load_sem.at[0])
    load_vals = pltpu.make_async_copy(colloc_hbm, vals, load_sem.at[1])
    load_place = pltpu.make_async_copy(place_hbm, place, load_sem.at[2])
    spans = [(s, min(DEPTH, total - s)) for s in range(0, total, DEPTH)]
    depth_loads = [
        pltpu.make_async_copy(
            coeffs_hbm.at[pl.ds(s, n)], coeffs.at[pl.ds(s, n)], depth_sem.at[i]
        )
        for i, (s, n) in enumerate(spans)
    ]
    load_vals.start()
    for load in depth_loads:
        load.start()
    load_core.start()
    load_place.start()

    barrier = pltpu.get_barrier_semaphore()
    def greet(sem, before):
        for t in range(gx_size):
            for g in range(gz_size):
                ahead = gx > t if before else gx < t

                @pl.when(ahead)
                def _():
                    pl.semaphore_signal(sem, inc=1, device_id=(t, gy, g), device_id_type=MESH)

        def inside(i):
            @pl.when(i < mine if before else i > mine)
            def _():
                pl.semaphore_signal(sem, inc=1, device_id=(gx, *seat(i)), device_id_type=MESH)

        sweep(inside)

    greet(barrier, False)

    @pl.when(gx * gz_size + mine > 0)
    def _():
        pl.semaphore_wait(barrier, gx * gz_size + mine)

    greet(ready.at[gx], True)

    def contract(first, last):
        acc = jnp.zeros((points, coeffs.shape[1]), F32)
        for i in range(first, last):
            s, n = spans[i]
            depth_loads[i].wait()
            acc += dot(vals[:, s : s + n], coeffs[s : s + n, :], 1, 0)
        return acc

    load_vals.wait()
    occ = contract(0, len(spans))
    occ = occ.astype(BF16)
    col_occ[own] = occ
    square = jnp.square(occ.astype(F32))
    high = square.astype(BF16)
    low = (square - high.astype(F32)).astype(BF16)
    ones = jnp.ones((8, occ.shape[1]), BF16)
    dens[gx] = (dot(ones, high, 1, 1) + dot(ones, low, 1, 1))[:1]
    for t in range(gx_size - 1):

        @pl.when(gx > t)
        def _():
            dens_copy(t).start()
            for k in range(halves):
                row_copy(t, k).start()


    @pl.when(mine < crowd - 1)
    def _():
        pl.semaphore_wait(ready.at[gx], crowd - 1 - mine)

    for h in sides:
        col_copy(h).start()
    if halves > 1:
        col_fwd(gy).start()
    for h in sides:
        col_win_copy(h).start()
    for h in range(gy_size):
        stage[h, :, :width] = vals[:, h * width : (h + 1) * width]
        if width < span:
            stage[h, :, width:] = jnp.zeros((points, span - width), BF16)
    for h in sides:
        cols_copy(h).start()
    own_cols = pltpu.make_async_copy(stage.at[gy], cols.at[gy], load_sem.at[3])
    own_cols.start()
    for t in range(1, gx_size):

        @pl.when(gx < t)
        def _():
            pl.semaphore_wait(ready.at[t], gz_size)
            dens_copy(t).start()
            for k in range(halves):
                row_copy(t, k).start()

    for h in sides:
        pl.semaphore_signal(known, inc=1, device_id=(gx, h, gz), device_id_type=MESH)
    col_win[gy] = vals[:, :lanes]
    load_core.wait()
    load_place.wait()
    spread = place[...]
    for k in range(halves):

        @pl.when(part == k)
        def _():
            starts = [a * points + k * half for a in range(gx_size)]
            core_q[...] = jnp.concatenate([core[:, s : s + half] for s in starts], axis=1)

    if sides:
        arrive(col_occ.at[pl.ds(0, len(sides))], col_sem)
    if halves > 1:
        for h in sides:
            col_fwd(h).start()
    if planes:
        arrive(dens.at[pl.ds(0, len(planes))], dens_sem)
    density = jnp.concatenate([dens[z] for z in range(gx_size)], axis=1)
    density = jnp.broadcast_to(density, (8, core.shape[1])).astype(BF16)
    potential = dot(density, core[...], 1, 1)[:1]
    pot_send[...] = potential
    for h, g in flat:
        pot_copy(h, g).start()

    if sides:
        arrive(col_win.at[pl.ds(0, len(sides))], col_win_sem)
    wins = dot(spread, col_win[...].reshape(side, lanes), 0, 1)
    win_t[...] = wins.reshape(win_t.shape)
    win_rows = wins.astype(BF16)

    if halves > 1:
        arrive(col_occ.at[pl.ds(0, gy_size)], col_sem, 1)
    for k in range(halves):
        row_occ[gx * halves + k] = col_occ[gy * halves + k, own_rows]
    for z in planes:
        arrive(row_occ.at[pl.ds(z * halves, halves)], row_sem, z)
    gram = None
    for k in range(halves):
        row_vals = [row_occ[z * halves + k] for z in range(gx_size)]
        col_vals = [col_occ[h * halves + k] for h in range(gy_size)]
        row_vals, col_vals = (jnp.concatenate(v, axis=0) for v in (row_vals, col_vals))
        term = dot(col_vals, row_vals, 1, 1)
        gram = term if gram is None else gram + term
    mixed = (core_q[...].astype(F32) * gram).astype(BF16)
    block = dot(win_rows, mixed, 1, 0)
    tight = win_t.shape[1]
    layers = tight // 8
    bands = []
    for j in range(layers):
        starts = [g * tight + j * 8 for g in range(gz_size)]
        bands.append(jnp.concatenate([block[at : at + 8] for at in starts], axis=0))
    for z in range(gx_size):
        pack = [band[:, z * half : (z + 1) * half] for band in bands]
        pack = jnp.concatenate(pack, axis=1).reshape(tot_send.shape[1:])
        tot_send[z] = pack.astype(BF16)
    if gy_size > 1:
        pl.semaphore_wait(known, gy_size - 1)
    for t in planes[::-1]:
        sweep(lambda i: tot_copy(t, *seat(i)).start())
    for h, g in flat:
        tot_copy(gx, h, g).start()
    own_tot = pltpu.make_async_copy(
        tot_send.at[gx, gz], tot_recv.at[gx * crowd + mine], tot_sem.at[1]
    )
    own_tot.start()

    if sides:
        arrive(cols.at[pl.ds(0, len(sides)), pl.ds(0, half)], cols_sem)
    if halves > 1:
        for h in sides:
            cols_fwd(h).start()

    spare = 8 - rows
    reach = z_send.shape[3]
    tail = span - reach

    def spread_out(index, left):
        gap = jnp.zeros((spare, side), F32)
        lines = []
        for a in range(gx_size):
            lines += [left[a * rows : (a + 1) * rows], gap]
        lefts = jnp.concatenate(lines, axis=0).astype(BF16)
        out = dot(lefts, cols[...].reshape(side, span), 1, 0).reshape(gx_size, 8, span)
        line = lax.broadcasted_iota(jnp.int32, (8, tail), 0)
        for a in range(gx_size):
            for j in range(reach // tail):
                block = out[a, :, j * tail : (j + 1) * tail]
                if j * spare < rows:
                    moved = pltpu.roll(out[a, :, reach:], (rows - j * spare) % 8, 0)
                    block = jnp.where(line < rows, block, moved)
                z_send[index, a, :, j * tail : (j + 1) * tail] = block.astype(BF16)
            if reach % tail:
                at = reach // tail * tail
                z_send[index, a, :, at:] = out[a, :, at:reach].astype(BF16)
        for t in planes[::-1]:
            z_copy(index, t).start()

    if flat:
        arrive(pot_recv.at[pl.ds(0, len(flat))], pot_sem)
    pot = pot_send[...]
    for h, g in flat:
        pot += pot_recv[h * gz_size + g]
    weighted = (win_t[gz] * pot).astype(BF16).astype(F32)
    own_cols.wait()
    if halves > 1 and sides:
        arrive(cols.at[pl.ds(0, len(sides)), pl.ds(0, half)], cols_sem, 1)
    spread_out(0, weighted)

    arrive(tot_recv, tot_sem)
    total_of = []
    for i in range(gy_size * halves):
        h, k = divmod(i, halves)
        slots = [
            z * crowd + h * gz_size + g
            for z in range(gx_size)
            for g in range(k, gz_size, halves)
        ]
        total_of.append(sum(tot_recv[slot].astype(F32) for slot in slots))
    owned = [
        jnp.concatenate([one[:, j * half : (j + 1) * half] for one in total_of], axis=1)
        for j in range(layers)
    ]
    owned = jnp.concatenate(owned, axis=0)
    spread_out(1, owned)

    if sides:
        leave(col_win.at[pl.ds(0, len(sides))], col_win_sem)
        leave(cols.at[pl.ds(0, len(sides))], cols_sem)
    if planes:
        leave(dens.at[pl.ds(0, len(planes))], dens_sem)
        leave(row_occ.at[pl.ds(0, len(planes) * halves)], row_sem)
    leave(col_occ.at[pl.ds(0, len(sides) + gy_size * (halves - 1))], col_sem)
    leave(pot_recv.at[pl.ds(0, len(flat))], pot_sem)
    leave(tot_recv.at[pl.ds(0, gx_size * crowd - 1)], tot_sem)

    for index in range(2):
        if planes:
            arrive(z_recv.at[index, pl.ds(0, len(planes))], z_sem, index)
        acc = z_send[index, gx].astype(F32)
        for z in planes:
            acc += z_recv[index, z].astype(F32)
        out_ref[index, :, :reach] = acc[:rows]
        for r in range(rows):
            j, k = divmod(r, spare)
            line = acc[rows + k : rows + k + 1, j * tail : j * tail + width - reach]
            out_ref[index, r : r + 1, reach:] = line

    if planes:
        leave(z_recv.at[:, pl.ds(0, len(planes))], z_sem)


def local(colloc, occ_coeffs, core):
    points, total = colloc.shape
    gx_size = lax.axis_size("gx")
    gy_size = lax.axis_size("gy")
    gz_size = lax.axis_size("gz")
    occupied = occ_coeffs.shape[1]
    rows = W // (gx_size * gz_size)
    width = total // gy_size
    row_count, flat = core.shape[0], core.shape[2]
    lanes = up(W, LANES)
    side = gy_size * points
    span = up(width, LANES)
    halves = 2 if gz_size % 2 == 0 else 1
    half = points // halves
    tiles = span // LANES
    spare = 8 - rows
    tail = max(t for t in range(1, tiles) if (tiles - t) // t * spare >= rows)
    reach = span - tail * LANES

    used = gx_size * rows
    tight = up(used, 8)
    place = np.zeros((lanes, gz_size, tight), np.float32)
    for a in range(gx_size):
        for g in range(gz_size):
            for k in range(rows):
                place[(a * gz_size + g) * rows + k, g, a * rows + k] = 1
    place = jnp.asarray(place.reshape(lanes, gz_size * tight), BF16)

    dims = (gx_size, gy_size, gz_size, rows, width)
    dma = pltpu.SemaphoreType.DMA
    vmem = pltpu.VMEM
    result = pl.pallas_call(
        functools.partial(kernel, dims),
        out_shape=pltpu.VMEM((2, rows, width), F32),
        in_specs=[pl.BlockSpec(memory_space=pltpu.HBM)] * 4,
        out_specs=pl.BlockSpec(memory_space=pltpu.VMEM),
        scratch_shapes=[
            vmem((points, total), BF16),
            vmem((total, occupied), BF16),
            vmem((row_count, flat), BF16),
            vmem(place.shape, BF16),
            vmem((row_count, gx_size * half), BF16),
            vmem((gx_size * halves, half, occupied), BF16),
            vmem((gy_size * halves, points, occupied), BF16),
            vmem((gy_size, points, lanes), BF16),
            vmem((gz_size, tight, side), F32),
            vmem((gx_size, 1, points), F32),
            vmem((gy_size, points, span), BF16),
            vmem((gy_size, points, span), BF16),
            vmem((1, side), F32),
            vmem((gy_size * gz_size, 1, side), F32),
            vmem((gx_size, gz_size, 8, tight // 8 * half), BF16),
            vmem((gx_size * gy_size * gz_size, 8, tight // 8 * half), BF16),
            vmem((2, gx_size, 8, reach), BF16),
            vmem((2, gx_size, 8, reach), BF16),
            dma((4,)),
            dma((-(-total // DEPTH),)),
            pltpu.SemaphoreType.REGULAR((gx_size,)),
            pltpu.SemaphoreType.REGULAR,
            dma((1 + gx_size,)),
            dma((3,)),
            dma((2,)),
            dma((2,)),
            dma((3,)),
            dma((2,)),
            dma((2,)),
            dma((3,)),
        ],
        compiler_params=pltpu.CompilerParams(
            collective_id=0, has_side_effects=True, vmem_limit_bytes=60 * 1024 * 1024
        ),
    )(colloc, occ_coeffs, core.reshape(row_count, flat), place)
    return result[0], result[1]


def solution(mesh):
    in_specs = (P(("gx", "gy"), None), P(None, "gz"), P("gx", "gy", None))
    out_specs = (P(("gx", "gz"), "gy"), P(("gx", "gz"), "gy"))
    return jax.shard_map(local, mesh=mesh, in_specs=in_specs, out_specs=out_specs, check_vma=False)
```

```python
import functools

import jax
import jax.numpy as jnp
import numpy as np
from jax import lax
from jax.experimental import pallas as pl
from jax.experimental.pallas import tpu as pltpu
from jax.sharding import PartitionSpec as P

W = 96
LANES = 128
DEPTH = 1024
MESH = pl.DeviceIdType.MESH
F32 = jnp.float32
BF16 = jnp.bfloat16


def up(value, step):
    return -(-value // step) * step


def dot(left, right, left_dim, right_dim):
    return lax.dot_general(
        left, right, (((left_dim,), (right_dim,)), ((), ())), preferred_element_type=F32
    )


def kernel(
    dims,
    colloc_hbm,
    coeffs_hbm,
    core_hbm,
    place_hbm,
    out_ref,
    vals,
    coeffs,
    core,
    place,
    core_q,
    row_occ,
    col_occ,
    col_win,
    win_t,
    dens,
    stage,
    cols,
    pot_send,
    pot_recv,
    tot_send,
    tot_recv,
    z_send,
    z_recv,
    load_sem,
    depth_sem,
    ready,
    known,
    row_sem,
    col_sem,
    col_win_sem,
    dens_sem,
    cols_sem,
    pot_sem,
    tot_sem,
    z_sem,
):
    gx_size, gy_size, gz_size, rows, width = dims
    gx, gy, gz = lax.axis_index("gx"), lax.axis_index("gy"), lax.axis_index("gz")
    points, total = vals.shape
    lanes = col_win.shape[2]
    crowd = gy_size * gz_size
    halves = 2 if gz_size % 2 == 0 else 1
    half = points // halves
    base = gz - lax.rem(gz, halves)
    span = cols.shape[2]
    side = gy_size * points
    part = lax.rem(gz, halves)

    def turn(pos, step, size):
        if size & (size - 1):
            return lax.rem(pos + step, size) if step else pos
        bit = 1
        while bit <= step:
            if step & bit:
                pos = pos + bit * (1 - 2 * lax.rem(lax.div(pos, bit), 2))
            bit *= 2
        return pos

    planes = [turn(gx, d, gx_size) for d in range(1, gx_size)]
    sides = [turn(gy, d, gy_size) for d in range(1, gy_size)]
    flat = [
        (turn(gy, dy, gy_size), turn(gz, dz, gz_size))
        for dy in range(gy_size)
        for dz in range(gz_size)
        if dy or dz
    ]
    mine = gy * gz_size + gz
    own = gy * halves + part
    mate = (gx, gy, base + halves - 1 - part)
    same = [
        (turn(gy, dy, gy_size), turn(gz, dz, gz_size))
        for dy in range(gy_size)
        for dz in range(0, gz_size, halves)
        if dy or dz
    ]

    def copy(src, dst, sems, target, slot=0):
        return pltpu.make_async_remote_copy(
            src_ref=src,
            dst_ref=dst,
            send_sem=sems.at[0],
            recv_sem=sems.at[1 + slot],
            device_id=target,
            device_id_type=MESH,
        )

    def arrive(ref, sems, slot=0):
        copy(ref, ref, sems, mate, slot).wait_recv()

    def leave(ref, sems):
        copy(ref, ref, sems, mate).wait_send()

    def seat(i):
        return lax.div(i, gz_size), lax.rem(i, gz_size)

    def sweep(body):
        if crowd <= 16:
            for i in range(crowd):
                body(jnp.int32(i))
        else:
            lax.fori_loop(0, crowd, lambda i, c: (body(i), c)[1], 0)

    own_rows = pl.ds(pl.multiple_of(part * half, half), half)

    def col_win_copy(h):
        return copy(vals.at[:, pl.ds(0, lanes)], col_win.at[gy], col_win_sem, (gx, h, gz))

    def dens_copy(t):
        some = dens.at[gx]
        return copy(some, some, dens_sem, (t, gy, gz))

    def row_copy(t, k):
        src = col_occ.at[own, pl.ds(k * half, half)]
        return copy(src, row_occ.at[gx * halves + part], row_sem, (t, gy, base + k), gx)

    def col_copy(h):
        some = col_occ.at[own]
        return copy(some, some, col_sem, (gx, h, gz))

    def col_fwd(h):
        some = col_occ.at[h * halves + part]
        return copy(some, some, col_sem, mate, 1)

    def cols_copy(h):
        at = pl.ds(pl.multiple_of(part * half, half), half)
        return copy(stage.at[h, at], cols.at[gy, at], cols_sem, (gx, h, gz))

    def cols_fwd(h):
        some = cols.at[h, pl.ds(pl.multiple_of(part * half, half), half)]
        return copy(some, some, cols_sem, mate, 1)

    def pot_copy(h, g):
        return copy(pot_send, pot_recv.at[mine], pot_sem, (gx, h, g))

    def tot_copy(t, h, g):
        return copy(tot_send.at[t, g], tot_recv.at[gx * crowd + mine], tot_sem, (t, h, g))

    def z_copy(index, t):
        return copy(z_send.at[index, t], z_recv.at[index, gx], z_sem, (t, gy, gz), index)

    load_core = pltpu.make_async_copy(core_hbm, core, load_sem.at[0])
    load_vals = pltpu.make_async_copy(colloc_hbm, vals, load_sem.at[1])
    load_place = pltpu.make_async_copy(place_hbm, place, load_sem.at[2])
    spans = [(s, min(DEPTH, total - s)) for s in range(0, total, DEPTH)]
    depth_loads = [
        pltpu.make_async_copy(
            coeffs_hbm.at[pl.ds(s, n)], coeffs.at[pl.ds(s, n)], depth_sem.at[i]
        )
        for i, (s, n) in enumerate(spans)
    ]
    load_vals.start()
    depth_loads[0].start()

    barrier = pltpu.get_barrier_semaphore()
    def greet(sem, before):
        for t in range(gx_size):

            @pl.when(gx > t if before else gx < t)
            def _():
                for k in range(halves):
                    pl.semaphore_signal(
                        sem, inc=1, device_id=(t, gy, base + k), device_id_type=MESH
                    )

        for h, g in same + [mate[1:]] * (halves - 1):
            i = h * gz_size + g

            @pl.when(i < mine if before else i > mine)
            def _():
                pl.semaphore_signal(sem, inc=1, device_id=(gx, h, g), device_id_type=MESH)

    greet(barrier, False)
    for load in depth_loads[1:]:
        load.start()
    load_core.start()
    load_place.start()
    below = lax.div(mine, halves) + part
    above = crowd // halves + halves - 2 - below

    @pl.when(gx + below > 0)
    def _():
        pl.semaphore_wait(barrier, gx * halves + below)

    greet(ready.at[gx], True)

    def contract(first, last):
        acc = jnp.zeros((points, coeffs.shape[1]), F32)
        for i in range(first, last):
            s, n = spans[i]
            depth_loads[i].wait()
            acc += dot(vals[:, s : s + n], coeffs[s : s + n, :], 1, 0)
        return acc

    load_vals.wait()
    occ = contract(0, len(spans))
    occ = occ.astype(BF16)
    col_occ[own] = occ
    square = jnp.square(occ.astype(F32))
    high = square.astype(BF16)
    low = (square - high.astype(F32)).astype(BF16)
    ones = jnp.ones((8, occ.shape[1]), BF16)
    dens[gx] = (dot(ones, high, 1, 1) + dot(ones, low, 1, 1))[:1]
    for t in range(gx_size - 1):

        @pl.when(gx > t)
        def _():
            dens_copy(t).start()
            for k in range(halves):
                row_copy(t, k).start()


    @pl.when(above > 0)
    def _():
        pl.semaphore_wait(ready.at[gx], above)

    for h in sides:
        col_copy(h).start()
    if halves > 1:
        col_fwd(gy).start()
    for h in sides:
        col_win_copy(h).start()
    for h in range(gy_size):
        stage[h, :, :width] = vals[:, h * width : (h + 1) * width]
        if width < span:
            stage[h, :, width:] = jnp.zeros((points, span - width), BF16)
    for h in sides:
        cols_copy(h).start()
    own_cols = pltpu.make_async_copy(stage.at[gy], cols.at[gy], load_sem.at[3])
    own_cols.start()
    for t in range(1, gx_size):

        @pl.when(gx < t)
        def _():
            pl.semaphore_wait(ready.at[t], halves)
            dens_copy(t).start()
            for k in range(halves):
                row_copy(t, k).start()

    for h, g in same:
        pl.semaphore_signal(known, inc=1, device_id=(gx, h, g), device_id_type=MESH)
    col_win[gy] = vals[:, :lanes]
    load_core.wait()
    load_place.wait()
    spread = place[...]
    for k in range(halves):

        @pl.when(part == k)
        def _():
            starts = [a * points + k * half for a in range(gx_size)]
            core_q[...] = jnp.concatenate([core[:, s : s + half] for s in starts], axis=1)

    if sides:
        arrive(col_occ.at[pl.ds(0, len(sides))], col_sem)
    if halves > 1:
        for h in sides:
            col_fwd(h).start()
    if planes:
        arrive(dens.at[pl.ds(0, len(planes))], dens_sem)
    density = jnp.concatenate([dens[z] for z in range(gx_size)], axis=1)
    density = jnp.broadcast_to(density, (8, core.shape[1])).astype(BF16)
    potential = dot(density, core[...], 1, 1)[:1]
    pot_send[...] = potential
    if same:
        pl.semaphore_wait(known, len(same))
    for h, g in flat:
        pot_copy(h, g).start()

    if sides:
        arrive(col_win.at[pl.ds(0, len(sides))], col_win_sem)
    wins = dot(spread, col_win[...].reshape(side, lanes), 0, 1)
    win_t[...] = wins.reshape(win_t.shape)
    win_rows = wins.astype(BF16)

    if halves > 1:
        arrive(col_occ.at[pl.ds(0, gy_size)], col_sem, 1)
    for k in range(halves):
        row_occ[gx * halves + k] = col_occ[gy * halves + k, own_rows]
    for z in planes:
        arrive(row_occ.at[pl.ds(z * halves, halves)], row_sem, z)
    gram = None
    for k in range(halves):
        row_vals = [row_occ[z * halves + k] for z in range(gx_size)]
        col_vals = [col_occ[h * halves + k] for h in range(gy_size)]
        row_vals, col_vals = (jnp.concatenate(v, axis=0) for v in (row_vals, col_vals))
        term = dot(col_vals, row_vals, 1, 1)
        gram = term if gram is None else gram + term
    mixed = (core_q[...].astype(F32) * gram).astype(BF16)
    block = dot(win_rows, mixed, 1, 0)
    tight = win_t.shape[1]
    layers = tight // 8
    bands = []
    for j in range(layers):
        starts = [g * tight + j * 8 for g in range(gz_size)]
        bands.append(jnp.concatenate([block[at : at + 8] for at in starts], axis=0))
    for z in reversed(range(gx_size)):
        pack = [band[:, z * half : (z + 1) * half] for band in bands]
        pack = jnp.concatenate(pack, axis=1).reshape(tot_send.shape[1:])
        tot_send[z] = pack.astype(BF16)

        @pl.when(gx != z)
        def _():
            sweep(lambda i: tot_copy(z, *seat(i)).start())

        @pl.when(gx == z)
        def _():
            for h, g in flat:
                tot_copy(z, h, g).start()

    own_tot = pltpu.make_async_copy(
        tot_send.at[gx, gz], tot_recv.at[gx * crowd + mine], tot_sem.at[1]
    )
    own_tot.start()

    if sides:
        arrive(cols.at[pl.ds(0, len(sides)), pl.ds(0, half)], cols_sem)
    if halves > 1:
        for h in sides:
            cols_fwd(h).start()

    spare = 8 - rows
    reach = z_send.shape[3]
    tail = span - reach

    def spread_out(index, left):
        gap = jnp.zeros((spare, side), F32)
        lines = []
        for a in range(gx_size):
            lines += [left[a * rows : (a + 1) * rows], gap]
        lefts = jnp.concatenate(lines, axis=0).astype(BF16)
        out = dot(lefts, cols[...].reshape(side, span), 1, 0).reshape(gx_size, 8, span)
        line = lax.broadcasted_iota(jnp.int32, (8, tail), 0)
        for a in range(gx_size):
            for j in range(reach // tail):
                block = out[a, :, j * tail : (j + 1) * tail]
                if j * spare < rows:
                    moved = pltpu.roll(out[a, :, reach:], (rows - j * spare) % 8, 0)
                    block = jnp.where(line < rows, block, moved)
                z_send[index, a, :, j * tail : (j + 1) * tail] = block.astype(BF16)
            if reach % tail:
                at = reach // tail * tail
                z_send[index, a, :, at:] = out[a, :, at:reach].astype(BF16)
        for t in range(gx_size):

            @pl.when(gx != t)
            def _():
                z_copy(index, t).start()

    if flat:
        arrive(pot_recv.at[pl.ds(0, len(flat))], pot_sem)
    pot = pot_send[...]
    for h, g in flat:
        pot += pot_recv[h * gz_size + g]
    weighted = (win_t[gz] * pot).astype(BF16).astype(F32)
    own_cols.wait()
    if halves > 1 and sides:
        arrive(cols.at[pl.ds(0, len(sides)), pl.ds(0, half)], cols_sem, 1)
    spread_out(0, weighted)

    arrive(tot_recv, tot_sem)
    total_of = []
    for i in range(gy_size * halves):
        h, k = divmod(i, halves)
        slots = [
            z * crowd + h * gz_size + g
            for z in range(gx_size)
            for g in range(k, gz_size, halves)
        ]
        total_of.append(sum(tot_recv[slot].astype(F32) for slot in slots))
    owned = [
        jnp.concatenate([one[:, j * half : (j + 1) * half] for one in total_of], axis=1)
        for j in range(layers)
    ]
    owned = jnp.concatenate(owned, axis=0)
    spread_out(1, owned)

    if sides:
        leave(col_win.at[pl.ds(0, len(sides))], col_win_sem)
        leave(cols.at[pl.ds(0, len(sides))], cols_sem)
    if planes:
        leave(dens.at[pl.ds(0, len(planes))], dens_sem)
        leave(row_occ.at[pl.ds(0, len(planes) * halves)], row_sem)
    leave(col_occ.at[pl.ds(0, len(sides) + gy_size * (halves - 1))], col_sem)
    leave(pot_recv.at[pl.ds(0, len(flat))], pot_sem)
    leave(tot_recv.at[pl.ds(0, gx_size * crowd - 1)], tot_sem)

    for index in range(2):
        if planes:
            arrive(z_recv.at[index, pl.ds(0, len(planes))], z_sem, index)
        acc = z_send[index, gx].astype(F32)
        for z in planes:
            acc += z_recv[index, z].astype(F32)
        out_ref[index, :, :reach] = acc[:rows]
        for r in range(rows):
            j, k = divmod(r, spare)
            line = acc[rows + k : rows + k + 1, j * tail : j * tail + width - reach]
            out_ref[index, r : r + 1, reach:] = line

    if planes:
        leave(z_recv.at[:, pl.ds(0, len(planes))], z_sem)


def local(colloc, occ_coeffs, core):
    points, total = colloc.shape
    gx_size = lax.axis_size("gx")
    gy_size = lax.axis_size("gy")
    gz_size = lax.axis_size("gz")
    occupied = occ_coeffs.shape[1]
    rows = W // (gx_size * gz_size)
    width = total // gy_size
    row_count, flat = core.shape[0], core.shape[2]
    lanes = up(W, LANES)
    side = gy_size * points
    span = up(width, LANES)
    halves = 2 if gz_size % 2 == 0 else 1
    half = points // halves
    tiles = span // LANES
    spare = 8 - rows
    tail = max(t for t in range(1, tiles) if (tiles - t) // t * spare >= rows)
    reach = span - tail * LANES

    used = gx_size * rows
    tight = up(used, 8)
    place = np.zeros((lanes, gz_size, tight), np.float32)
    for a in range(gx_size):
        for g in range(gz_size):
            for k in range(rows):
                place[(a * gz_size + g) * rows + k, g, a * rows + k] = 1
    place = jnp.asarray(place.reshape(lanes, gz_size * tight), BF16)

    dims = (gx_size, gy_size, gz_size, rows, width)
    dma = pltpu.SemaphoreType.DMA
    vmem = pltpu.VMEM
    result = pl.pallas_call(
        functools.partial(kernel, dims),
        out_shape=pltpu.VMEM((2, rows, width), F32),
        in_specs=[pl.BlockSpec(memory_space=pltpu.HBM)] * 4,
        out_specs=pl.BlockSpec(memory_space=pltpu.VMEM),
        scratch_shapes=[
            vmem((points, total), BF16),
            vmem((total, occupied), BF16),
            vmem((row_count, flat), BF16),
            vmem(place.shape, BF16),
            vmem((row_count, gx_size * half), BF16),
            vmem((gx_size * halves, half, occupied), BF16),
            vmem((gy_size * halves, points, occupied), BF16),
            vmem((gy_size, points, lanes), BF16),
            vmem((gz_size, tight, side), F32),
            vmem((gx_size, 1, points), F32),
            vmem((gy_size, points, span), BF16),
            vmem((gy_size, points, span), BF16),
            vmem((1, side), F32),
            vmem((gy_size * gz_size, 1, side), F32),
            vmem((gx_size, gz_size, 8, tight // 8 * half), BF16),
            vmem((gx_size * gy_size * gz_size, 8, tight // 8 * half), BF16),
            vmem((2, gx_size, 8, reach), BF16),
            vmem((2, gx_size, 8, reach), BF16),
            dma((4,)),
            dma((-(-total // DEPTH),)),
            pltpu.SemaphoreType.REGULAR((gx_size,)),
            pltpu.SemaphoreType.REGULAR,
            dma((1 + gx_size,)),
            dma((3,)),
            dma((2,)),
            dma((2,)),
            dma((3,)),
            dma((2,)),
            dma((2,)),
            dma((3,)),
        ],
        compiler_params=pltpu.CompilerParams(
            collective_id=0, has_side_effects=True, vmem_limit_bytes=60 * 1024 * 1024
        ),
    )(colloc, occ_coeffs, core.reshape(row_count, flat), place)
    return result[0], result[1]


def solution(mesh):
    in_specs = (P(("gx", "gy"), None), P(None, "gz"), P("gx", "gy", None))
    out_specs = (P(("gx", "gz"), "gy"), P(("gx", "gz"), "gy"))
    return jax.shard_map(local, mesh=mesh, in_specs=in_specs, out_specs=out_specs, check_vma=False)
```

```python
import functools

import jax
import jax.numpy as jnp
import numpy as np
from jax import lax
from jax.experimental import pallas as pl
from jax.experimental.pallas import tpu as pltpu
from jax.sharding import PartitionSpec as P

W = 96
LANES = 128
DEPTH = 1024
MESH = pl.DeviceIdType.MESH
F32 = jnp.float32
BF16 = jnp.bfloat16


def up(value, step):
    return -(-value // step) * step


def dot(left, right, left_dim, right_dim):
    return lax.dot_general(
        left, right, (((left_dim,), (right_dim,)), ((), ())), preferred_element_type=F32
    )


def kernel(
    dims,
    colloc_hbm,
    coeffs_hbm,
    core_hbm,
    place_hbm,
    out_ref,
    vals,
    coeffs,
    core,
    place,
    core_q,
    cores,
    core_t,
    row_win,
    back,
    row_occ,
    col_occ,
    col_win,
    win_t,
    dens,
    stage,
    cols,
    pot_send,
    pot_recv,
    tot_send,
    tot_recv,
    back_send,
    back_recv,
    z_send,
    z_recv,
    load_sem,
    depth_sem,
    ready,
    known,
    row_sem,
    core_sem,
    row_win_sem,
    col_sem,
    col_win_sem,
    dens_sem,
    cols_sem,
    cols_fwd_sem,
    pot_sem,
    tot_sem,
    back_sem,
    z_sem,
):
    gx_size, gy_size, gz_size, rows, width = dims
    gx, gy, gz = lax.axis_index("gx"), lax.axis_index("gy"), lax.axis_index("gz")
    points, total = vals.shape
    lanes = col_win.shape[2]
    crowd = gy_size * gz_size
    halves = 2 if gz_size % 2 == 0 else 1
    half = points // halves
    base = gz - lax.rem(gz, halves)
    span = cols.shape[2]
    side = gy_size * points
    part = lax.rem(gz, halves)

    def turn(pos, step, size):
        if size & (size - 1):
            return lax.rem(pos + step, size) if step else pos
        bit = 1
        while bit <= step:
            if step & bit:
                pos = pos + bit * (1 - 2 * lax.rem(lax.div(pos, bit), 2))
            bit *= 2
        return pos

    planes = [turn(gx, d, gx_size) for d in range(1, gx_size)]
    sides = [turn(gy, d, gy_size) for d in range(1, gy_size)]
    flat = [
        (turn(gy, dy, gy_size), turn(gz, dz, gz_size))
        for dy in range(gy_size)
        for dz in range(gz_size)
        if dy or dz
    ]
    across = [(gy, base + k) for k in range(halves)] + [(h, gz) for h in sides]
    mine = gy * gz_size + gz
    own = gy * halves + part
    mate = (gx, gy, base + halves - 1 - part)
    same = [
        (turn(gy, dy, gy_size), turn(gz, dz, gz_size))
        for dy in range(gy_size)
        for dz in range(0, gz_size, halves)
        if dy or dz
    ]

    def copy(src, dst, sems, target, slot=0):
        return pltpu.make_async_remote_copy(
            src_ref=src,
            dst_ref=dst,
            send_sem=sems.at[0],
            recv_sem=sems.at[1 + slot],
            device_id=target,
            device_id_type=MESH,
        )

    def arrive(ref, sems, slot=0):
        copy(ref, ref, sems, mate, slot).wait_recv()

    def leave(ref, sems):
        copy(ref, ref, sems, mate).wait_send()

    def lane_copy(src, dst, sems, t, target):
        return pltpu.make_async_remote_copy(
            src_ref=src,
            dst_ref=dst,
            send_sem=sems.at[0, t],
            recv_sem=sems.at[1, gx],
            device_id=target,
            device_id_type=MESH,
        )

    def lane_wait(ref, sems, z):
        pltpu.make_async_remote_copy(
            src_ref=ref,
            dst_ref=ref,
            send_sem=sems.at[0, z],
            recv_sem=sems.at[1, z],
            device_id=mate,
            device_id_type=MESH,
        ).wait_recv()

    def lane_leave(ref, sems, t):
        pltpu.make_async_remote_copy(
            src_ref=ref,
            dst_ref=ref,
            send_sem=sems.at[0, t],
            recv_sem=sems.at[1, t],
            device_id=mate,
            device_id_type=MESH,
        ).wait_send()

    steps = range(1, gx_size)

    def other(d):
        return gx + d if d % 2 else gx - d

    def keeper(d):
        return gx - d if d % 2 else gx + d

    def inside(t):
        return (t >= 0) & (t < gx_size)

    def kept_by(z):
        gap = gx - z
        odd = lax.rem(jnp.abs(gap), 2)
        return ((gap > 0) & (odd == 1)) | ((gap < 0) & (odd == 0))

    def seat(i):
        return lax.div(i, gz_size), lax.rem(i, gz_size)

    def sweep(body):
        if crowd <= 16:
            for i in range(crowd):
                body(jnp.int32(i))
        else:
            lax.fori_loop(0, crowd, lambda i, c: (body(i), c)[1], 0)

    own_rows = pl.ds(pl.multiple_of(part * half, half), half)

    def col_win_copy(h):
        return copy(vals.at[:, pl.ds(0, lanes)], col_win.at[gy], col_win_sem, (gx, h, gz))

    def dens_copy(t):
        some = dens.at[gx]
        return copy(some, some, dens_sem, (t, gy, gz))

    def row_copy(t, k):
        src = col_occ.at[own, pl.ds(k * half, half)]
        return lane_copy(src, row_occ.at[gx * halves + part], row_sem, t, (t, gy, base + k))

    def core_copy(t, h):
        src = cores.at[t, pl.ds(pl.multiple_of(h * points + part * half, half), half)]
        return lane_copy(src, core_t.at[gx, gy], core_sem, t, (t, h, gz))

    def row_win_copy(t):
        src = vals.at[own_rows, pl.ds(0, lanes)]
        return lane_copy(src, row_win.at[gx], row_win_sem, t, (t, gy, gz))

    def lend(t):
        row_win_copy(t).start()
        for h in range(gy_size):
            core_copy(t, h).start()

    def col_copy(h):
        some = col_occ.at[own]
        return copy(some, some, col_sem, (gx, h, gz))

    def col_fwd(h):
        some = col_occ.at[h * halves + part]
        return copy(some, some, col_sem, mate, 1)

    def cols_copy(h):
        return copy(stage.at[h], cols.at[gy], cols_sem, (gx, h, gz))

    def cols_fwd(h):
        some = cols.at[h]
        return copy(some, some, cols_fwd_sem, mate)

    def pot_copy(h, g):
        return copy(pot_send, pot_recv.at[mine], pot_sem, (gx, h, g))

    def tot_copy(t, h, g):
        dst = tot_recv.at[gx * crowd + mine]
        return lane_copy(tot_send.at[t, g], dst, tot_sem, t, (t, h, g))

    def back_copy(h, g):
        return copy(back_send.at[g], back_recv.at[mine], back_sem, (gx, h, g))

    def z_copy(index, t):
        return copy(z_send.at[index, t], z_recv.at[index, gx], z_sem, (t, gy, gz), index)

    load_core = pltpu.make_async_copy(core_hbm, core, load_sem.at[0])
    load_vals = pltpu.make_async_copy(colloc_hbm, vals, load_sem.at[1])
    load_place = pltpu.make_async_copy(place_hbm, place, load_sem.at[2])
    spans = [(s, min(DEPTH, total - s)) for s in range(0, total, DEPTH)]
    depth_loads = [
        pltpu.make_async_copy(
            coeffs_hbm.at[pl.ds(s, n)], coeffs.at[pl.ds(s, n)], depth_sem.at[i]
        )
        for i, (s, n) in enumerate(spans)
    ]
    load_core.start()
    load_vals.start()
    depth_loads[0].start()

    barrier = pltpu.get_barrier_semaphore()
    def greet(sem, before):
        for t in range(gx_size):

            @pl.when(gx > t if before else gx < t)
            def _():
                for h, g in across:
                    pl.semaphore_signal(sem, inc=1, device_id=(t, h, g), device_id_type=MESH)

        for h, g in same + [mate[1:]] * (halves - 1):
            i = h * gz_size + g

            @pl.when(i < mine if before else i > mine)
            def _():
                pl.semaphore_signal(sem, inc=1, device_id=(gx, h, g), device_id_type=MESH)

    greet(barrier, False)
    for load in depth_loads[1:]:
        load.start()
    load_place.start()
    below = lax.div(mine, halves) + part
    above = crowd // halves + halves - 2 - below

    @pl.when(gx + below > 0)
    def _():
        pl.semaphore_wait(barrier, gx * len(across) + below)

    greet(ready.at[gx], True)

    def contract(first, last):
        acc = jnp.zeros((points, coeffs.shape[1]), F32)
        for i in range(first, last):
            s, n = spans[i]
            depth_loads[i].wait()
            acc += dot(vals[:, s : s + n], coeffs[s : s + n, :], 1, 0)
        return acc

    load_vals.wait()
    early = len(spans) // 2
    occ = contract(0, early)
    load_core.wait()
    for a in range(gx_size):
        cores[a] = core[:, a * points : (a + 1) * points]
    for d in steps[::2]:

        @pl.when(gx >= d)
        def _():
            lend(gx - d)

    occ += contract(early, len(spans))
    occ = occ.astype(BF16)
    col_occ[own] = occ
    square = jnp.square(occ.astype(F32))
    high = square.astype(BF16)
    low = (square - high.astype(F32)).astype(BF16)
    ones = jnp.ones((8, occ.shape[1]), BF16)
    dens[gx] = (dot(ones, high, 1, 1) + dot(ones, low, 1, 1))[:1]

    @pl.when(above > 0)
    def _():
        pl.semaphore_wait(ready.at[gx], above)

    if halves > 1:
        col_fwd(gy).start()
    for h in sides:
        col_copy(h).start()
    for t in range(gx_size - 1):

        @pl.when(gx > t)
        def _():
            dens_copy(t).start()

        @pl.when((gx > t) & (lax.rem(jnp.abs(gx - t), 2) == 1))
        def _():
            for k in range(halves):
                row_copy(t, k).start()

    for h in sides:
        col_win_copy(h).start()
    for h in range(gy_size):
        stage[h, :, :width] = vals[:, h * width : (h + 1) * width]
        if width < span:
            stage[h, :, width:] = jnp.zeros((points, span - width), BF16)
    lead = part == halves - 1

    @pl.when(lead)
    def _():
        for h in sides:
            cols_copy(h).start()

    own_cols = pltpu.make_async_copy(stage.at[gy], cols.at[gy], load_sem.at[3])
    own_cols.start()
    for t in range(1, gx_size):

        @pl.when(gx < t)
        def _():
            pl.semaphore_wait(ready.at[t], len(across))
            dens_copy(t).start()

        @pl.when((gx < t) & (lax.rem(jnp.abs(gx - t), 2) == 0))
        def _():
            lend(t)
            for k in range(halves):
                row_copy(t, k).start()

    for h, g in same:
        pl.semaphore_signal(known, inc=1, device_id=(gx, h, g), device_id_type=MESH)
    col_win[gy] = vals[:, :lanes]
    load_place.wait()
    back[...] = jnp.zeros(back.shape, F32)
    for z in range(gx_size):

        @pl.when((gx != z) & jnp.logical_not(kept_by(z)))
        def _():
            tot_recv[pl.ds(z * crowd, crowd)] = jnp.zeros((crowd, *tot_recv.shape[1:]), BF16)

    spread = place[...]
    for k in range(halves):

        @pl.when(part == k)
        def _():
            for a in range(gx_size):
                core_q[a] = core[:, a * points + k * half : a * points + (k + 1) * half]

    if sides:
        arrive(col_occ.at[pl.ds(0, len(sides))], col_sem)
    if halves > 1:
        for h in sides:
            col_fwd(h).start()
    if planes:
        arrive(dens.at[pl.ds(0, len(planes))], dens_sem)
    density = jnp.concatenate([dens[z] for z in range(gx_size)], axis=1)
    density = jnp.broadcast_to(density, (8, core.shape[1])).astype(BF16)
    potential = dot(density, core[...], 1, 1)[:1]
    pot_send[...] = potential
    if same:
        pl.semaphore_wait(known, len(same))
    for h, g in flat:
        pot_copy(h, g).start()

    if sides:
        arrive(col_win.at[pl.ds(0, len(sides))], col_win_sem)
    wins = dot(spread, col_win[...].reshape(side, lanes), 0, 1)
    win_t[...] = wins.reshape(win_t.shape)
    win_rows = wins.astype(BF16)

    if halves > 1:
        arrive(col_occ.at[pl.ds(0, gy_size)], col_sem, 1)
    for k in range(halves):
        row_occ[gx * halves + k] = col_occ[gy * halves + k, own_rows]
    tight = win_t.shape[1]
    layers = tight // 8

    def side_occ(k):
        return jnp.concatenate([col_occ[h * halves + k] for h in range(gy_size)], axis=0)

    def forward(z):
        gram = None
        for k in range(halves):
            term = dot(side_occ(k), row_occ[z * halves + k], 1, 1)
            gram = term if gram is None else gram + term
        mixed = (core_q[z].astype(F32) * gram).astype(BF16)
        block = dot(win_rows, mixed, 1, 0)
        pack = []
        for j in range(layers):
            starts = [g * tight + j * 8 for g in range(gz_size)]
            pack.append(jnp.concatenate([block[at : at + 8] for at in starts], axis=0))
        pack = jnp.concatenate(pack, axis=1).reshape(tot_send.shape[1:])
        tot_send[z] = pack.astype(BF16)

    def backward(z):
        gram = None
        for k in range(halves):
            term = dot(row_occ[z * halves + k], side_occ(k), 1, 1)
            gram = term if gram is None else gram + term
        core_vals = jnp.concatenate([core_t[z, h].astype(F32) for h in range(gy_size)], axis=1)
        mixed = (core_vals * gram).astype(BF16)
        far_win = dot(spread, row_win[z], 0, 1).astype(BF16)
        back[...] += dot(far_win, mixed, 1, 0)

    forward(gx)
    for h, g in flat:
        tot_copy(gx, h, g).start()
    own_tot = pltpu.make_async_copy(
        tot_send.at[gx, gz], tot_recv.at[gx * crowd + mine], tot_sem.at[1, gx]
    )
    own_tot.start()
    for d in steps:
        z = other(d)

        @pl.when(inside(z))
        def _():
            lane_wait(row_occ.at[pl.ds(z * halves, halves)], row_sem, z)
            lane_wait(row_win.at[z], row_win_sem, z)
            lane_wait(core_t.at[z], core_sem, z)
            forward(z)
            sweep(lambda i: tot_copy(z, *seat(i)).start())
            backward(z)

    back_send[...] = back[...].reshape(back_send.shape).astype(BF16)
    for h, g in flat:
        back_copy(h, g).start()
    own_back = pltpu.make_async_copy(back_send.at[gz], back_recv.at[mine], back_sem.at[1])
    own_back.start()

    if sides:

        @pl.when(lead)
        def _():
            arrive(cols.at[pl.ds(0, len(sides))], cols_sem)
            if halves > 1:
                for h in sides:
                    cols_fwd(h).start()

    spare = 8 - rows
    reach = z_send.shape[3]
    tail = span - reach

    def spread_out(index, left):
        gap = jnp.zeros((spare, side), F32)
        lines = []
        for a in range(gx_size):
            lines += [left[a * rows : (a + 1) * rows], gap]
        lefts = jnp.concatenate(lines, axis=0).astype(BF16)
        out = dot(lefts, cols[...].reshape(side, span), 1, 0).reshape(gx_size, 8, span)
        line = lax.broadcasted_iota(jnp.int32, (8, tail), 0)
        for a in range(gx_size):
            for j in range(reach // tail):
                block = out[a, :, j * tail : (j + 1) * tail]
                if j * spare < rows:
                    moved = pltpu.roll(out[a, :, reach:], (rows - j * spare) % 8, 0)
                    block = jnp.where(line < rows, block, moved)
                z_send[index, a, :, j * tail : (j + 1) * tail] = block.astype(BF16)
            if reach % tail:
                at = reach // tail * tail
                z_send[index, a, :, at:] = out[a, :, at:reach].astype(BF16)
        for t in range(gx_size):

            @pl.when(gx != t)
            def _():
                z_copy(index, t).start()

    if flat:
        arrive(pot_recv.at[pl.ds(0, len(flat))], pot_sem)
    pot = pot_send[...]
    for h, g in flat:
        pot += pot_recv[h * gz_size + g]
    weighted = (win_t[gz] * pot).astype(BF16).astype(F32)
    own_cols.wait()
    if halves > 1 and sides:

        @pl.when(part == 0)
        def _():
            arrive(cols.at[pl.ds(0, len(sides))], cols_fwd_sem)

    spread_out(0, weighted)

    arrive(back_recv, back_sem)
    for z in range(gx_size):

        @pl.when((gx == z) | kept_by(z))
        def _():
            lane_wait(tot_recv.at[pl.ds(z * crowd, crowd)], tot_sem, z)

    total_of = []
    for i in range(gy_size * halves):
        h, k = divmod(i, halves)
        slots = [
            z * crowd + h * gz_size + g
            for z in range(gx_size)
            for g in range(k, gz_size, halves)
        ]
        total_of.append(sum(tot_recv[slot].astype(F32) for slot in slots))
    owned = [
        jnp.concatenate([one[:, j * half : (j + 1) * half] for one in total_of], axis=1)
        for j in range(layers)
    ]
    owned = jnp.concatenate(owned, axis=0)
    owned += sum(back_recv[i].astype(F32) for i in range(crowd)).reshape(owned.shape)
    spread_out(1, owned)

    if sides:
        leave(col_win.at[pl.ds(0, len(sides))], col_win_sem)

        @pl.when(lead)
        def _():
            leave(cols.at[pl.ds(0, len(sides))], cols_sem)
            if halves > 1:
                leave(cols.at[pl.ds(0, len(sides))], cols_fwd_sem)

    if planes:
        leave(dens.at[pl.ds(0, len(planes))], dens_sem)
    leave(col_occ.at[pl.ds(0, len(sides) + gy_size * (halves - 1))], col_sem)
    leave(pot_recv.at[pl.ds(0, len(flat))], pot_sem)
    leave(back_recv.at[pl.ds(0, len(flat))], back_sem)
    lane_leave(tot_recv.at[pl.ds(0, len(flat))], tot_sem, gx)
    for d in steps:
        t, z = keeper(d), other(d)

        @pl.when(inside(t))
        def _():
            lane_leave(row_occ.at[pl.ds(0, halves)], row_sem, t)
            lane_leave(row_win.at[0], row_win_sem, t)
            lane_leave(core_t.at[0], core_sem, t)

        @pl.when(inside(z))
        def _():
            lane_leave(tot_recv.at[pl.ds(0, crowd)], tot_sem, z)


    for index in range(2):
        if planes:
            arrive(z_recv.at[index, pl.ds(0, len(planes))], z_sem, index)
        acc = z_send[index, gx].astype(F32)
        for z in planes:
            acc += z_recv[index, z].astype(F32)
        out_ref[index, :, :reach] = acc[:rows]
        for r in range(rows):
            j, k = divmod(r, spare)
            line = acc[rows + k : rows + k + 1, j * tail : j * tail + width - reach]
            out_ref[index, r : r + 1, reach:] = line

    if planes:
        leave(z_recv.at[:, pl.ds(0, len(planes))], z_sem)


def local(colloc, occ_coeffs, core):
    points, total = colloc.shape
    gx_size = lax.axis_size("gx")
    gy_size = lax.axis_size("gy")
    gz_size = lax.axis_size("gz")
    occupied = occ_coeffs.shape[1]
    rows = W // (gx_size * gz_size)
    width = total // gy_size
    row_count, flat = core.shape[0], core.shape[2]
    lanes = up(W, LANES)
    side = gy_size * points
    span = up(width, LANES)
    halves = 2 if gz_size % 2 == 0 else 1
    half = points // halves
    tiles = span // LANES
    spare = 8 - rows
    tail = max(t for t in range(1, tiles) if (tiles - t) // t * spare >= rows)
    reach = span - tail * LANES

    used = gx_size * rows
    tight = up(used, 8)
    place = np.zeros((lanes, gz_size, tight), np.float32)
    for a in range(gx_size):
        for g in range(gz_size):
            for k in range(rows):
                place[(a * gz_size + g) * rows + k, g, a * rows + k] = 1
    place = jnp.asarray(place.reshape(lanes, gz_size * tight), BF16)

    dims = (gx_size, gy_size, gz_size, rows, width)
    dma = pltpu.SemaphoreType.DMA
    vmem = pltpu.VMEM
    result = pl.pallas_call(
        functools.partial(kernel, dims),
        out_shape=pltpu.VMEM((2, rows, width), F32),
        in_specs=[pl.BlockSpec(memory_space=pltpu.HBM)] * 4,
        out_specs=pl.BlockSpec(memory_space=pltpu.VMEM),
        scratch_shapes=[
            vmem((points, total), BF16),
            vmem((total, occupied), BF16),
            vmem((row_count, flat), BF16),
            vmem(place.shape, BF16),
            vmem((gx_size, row_count, half), BF16),
            vmem((gx_size, row_count, points), BF16),
            vmem((gx_size, gy_size, half, points), BF16),
            vmem((gx_size, half, lanes), BF16),
            vmem((gz_size * tight, side), F32),
            vmem((gx_size * halves, half, occupied), BF16),
            vmem((gy_size * halves, points, occupied), BF16),
            vmem((gy_size, points, lanes), BF16),
            vmem((gz_size, tight, side), F32),
            vmem((gx_size, 1, points), F32),
            vmem((gy_size, points, span), BF16),
            vmem((gy_size, points, span), BF16),
            vmem((1, side), F32),
            vmem((gy_size * gz_size, 1, side), F32),
            vmem((gx_size, gz_size, 8, tight // 8 * half), BF16),
            vmem((gx_size * gy_size * gz_size, 8, tight // 8 * half), BF16),
            vmem((gz_size, tight // 8, 8, side), BF16),
            vmem((gy_size * gz_size, tight // 8, 8, side), BF16),
            vmem((2, gx_size, 8, reach), BF16),
            vmem((2, gx_size, 8, reach), BF16),
            dma((4,)),
            dma((-(-total // DEPTH),)),
            pltpu.SemaphoreType.REGULAR((gx_size,)),
            pltpu.SemaphoreType.REGULAR,
            dma((2, gx_size)),
            dma((2, gx_size)),
            dma((2, gx_size)),
            dma((3,)),
            dma((2,)),
            dma((2,)),
            dma((2,)),
            dma((2,)),
            dma((2,)),
            dma((2, gx_size)),
            dma((2,)),
            dma((3,)),
        ],
        compiler_params=pltpu.CompilerParams(
            collective_id=0, has_side_effects=True, vmem_limit_bytes=60 * 1024 * 1024
        ),
    )(colloc, occ_coeffs, core.reshape(row_count, flat), place)
    return result[0], result[1]


def solution(mesh):
    in_specs = (P(("gx", "gy"), None), P(None, "gz"), P("gx", "gy", None))
    out_specs = (P(("gx", "gz"), "gy"), P(("gx", "gz"), "gy"))
    return jax.shard_map(local, mesh=mesh, in_specs=in_specs, out_specs=out_specs, check_vma=False)
```

```python
import functools

import jax
import jax.numpy as jnp
import numpy as np
from jax import lax
from jax.experimental import pallas as pl
from jax.experimental.pallas import tpu as pltpu
from jax.sharding import PartitionSpec as P

W = 96
LANES = 128
DEPTH = 1024
MESH = pl.DeviceIdType.MESH
F32 = jnp.float32
BF16 = jnp.bfloat16


def up(value, step):
    return -(-value // step) * step


def dot(left, right, left_dim, right_dim):
    return lax.dot_general(
        left, right, (((left_dim,), (right_dim,)), ((), ())), preferred_element_type=F32
    )


def kernel(
    dims,
    colloc_hbm,
    coeffs_hbm,
    core_hbm,
    place_hbm,
    out_ref,
    vals,
    coeffs,
    core,
    place,
    core_q,
    cores,
    core_t,
    row_win,
    row_occ,
    col_occ,
    col_win,
    win_t,
    dens,
    stage,
    cols,
    pot_send,
    pot_recv,
    tot_send,
    tot_recv,
    back_send,
    back_recv,
    z_send,
    z_recv,
    load_sem,
    depth_sem,
    ready,
    known,
    row_sem,
    core_sem,
    row_win_sem,
    col_sem,
    col_win_sem,
    dens_sem,
    cols_sem,
    cols_fwd_sem,
    pot_sem,
    tot_sem,
    back_sem,
    z_sem,
):
    gx_size, gy_size, gz_size, rows, width = dims
    gx, gy, gz = lax.axis_index("gx"), lax.axis_index("gy"), lax.axis_index("gz")
    points, total = vals.shape
    lanes = col_win.shape[2]
    crowd = gy_size * gz_size
    halves = 2 if gz_size % 2 == 0 else 1
    half = points // halves
    base = gz - lax.rem(gz, halves)
    span = cols.shape[2]
    side = gy_size * points
    part = lax.rem(gz, halves)

    def turn(pos, step, size):
        if size & (size - 1):
            return lax.rem(pos + step, size) if step else pos
        bit = 1
        while bit <= step:
            if step & bit:
                pos = pos + bit * (1 - 2 * lax.rem(lax.div(pos, bit), 2))
            bit *= 2
        return pos

    planes = [turn(gx, d, gx_size) for d in range(1, gx_size)]
    sides = [turn(gy, d, gy_size) for d in range(1, gy_size)]
    flat = [
        (turn(gy, dy, gy_size), turn(gz, dz, gz_size))
        for dy in range(gy_size)
        for dz in range(gz_size)
        if dy or dz
    ]
    across = [(gy, base + k) for k in range(halves)] + [(h, gz) for h in sides]
    mine = gy * gz_size + gz
    own = gy * halves + part
    mate = (gx, gy, base + halves - 1 - part)
    same = [
        (turn(gy, dy, gy_size), turn(gz, dz, gz_size))
        for dy in range(gy_size)
        for dz in range(0, gz_size, halves)
        if dy or dz
    ]

    def copy(src, dst, sems, target, slot=0):
        return pltpu.make_async_remote_copy(
            src_ref=src,
            dst_ref=dst,
            send_sem=sems.at[0],
            recv_sem=sems.at[1 + slot],
            device_id=target,
            device_id_type=MESH,
        )

    def arrive(ref, sems, slot=0):
        copy(ref, ref, sems, mate, slot).wait_recv()

    def leave(ref, sems):
        copy(ref, ref, sems, mate).wait_send()

    def lane_copy(src, dst, sems, t, target):
        return pltpu.make_async_remote_copy(
            src_ref=src,
            dst_ref=dst,
            send_sem=sems.at[0, t],
            recv_sem=sems.at[1, gx],
            device_id=target,
            device_id_type=MESH,
        )

    def lane_wait(ref, sems, z):
        pltpu.make_async_remote_copy(
            src_ref=ref,
            dst_ref=ref,
            send_sem=sems.at[0, z],
            recv_sem=sems.at[1, z],
            device_id=mate,
            device_id_type=MESH,
        ).wait_recv()

    def lane_leave(ref, sems, t):
        pltpu.make_async_remote_copy(
            src_ref=ref,
            dst_ref=ref,
            send_sem=sems.at[0, t],
            recv_sem=sems.at[1, t],
            device_id=mate,
            device_id_type=MESH,
        ).wait_send()

    steps = range(1, gx_size)

    def other(d):
        return gx + d if d % 2 else gx - d

    def keeper(d):
        return gx - d if d % 2 else gx + d

    def inside(t):
        return (t >= 0) & (t < gx_size)

    def keeps(z):
        gap = z - gx
        odd = lax.rem(jnp.abs(gap), 2)
        return ((gap > 0) & (odd == 1)) | ((gap < 0) & (odd == 0))

    def kept_by(z):
        gap = gx - z
        odd = lax.rem(jnp.abs(gap), 2)
        return ((gap > 0) & (odd == 1)) | ((gap < 0) & (odd == 0))

    def seat(i):
        return lax.div(i, gz_size), lax.rem(i, gz_size)

    def sweep(body):
        if crowd <= 16:
            for i in range(crowd):
                body(jnp.int32(i))
        else:
            lax.fori_loop(0, crowd, lambda i, c: (body(i), c)[1], 0)

    own_rows = pl.ds(pl.multiple_of(part * half, half), half)

    def col_win_copy(h):
        return copy(vals.at[:, pl.ds(0, lanes)], col_win.at[gy], col_win_sem, (gx, h, gz))

    def dens_copy(t):
        some = dens.at[gx]
        return copy(some, some, dens_sem, (t, gy, gz))

    def row_copy(t, k):
        src = col_occ.at[own, pl.ds(k * half, half)]
        return lane_copy(src, row_occ.at[gx * halves + part], row_sem, t, (t, gy, base + k))

    def core_copy(t, h):
        src = cores.at[t, pl.ds(pl.multiple_of(h * points + part * half, half), half)]
        return lane_copy(src, core_t.at[gx, gy], core_sem, t, (t, h, gz))

    def row_win_copy(t):
        src = vals.at[own_rows, pl.ds(0, lanes)]
        return lane_copy(src, row_win.at[gx], row_win_sem, t, (t, gy, gz))

    def lend(t):
        row_win_copy(t).start()
        for h in range(gy_size):
            core_copy(t, h).start()

    def col_copy(h):
        some = col_occ.at[own]
        return copy(some, some, col_sem, (gx, h, gz))

    def col_fwd(h):
        some = col_occ.at[h * halves + part]
        return copy(some, some, col_sem, mate, 1)

    def cols_copy(h):
        return copy(stage.at[h], cols.at[gy], cols_sem, (gx, h, gz))

    def cols_fwd(h):
        some = cols.at[h]
        return copy(some, some, cols_fwd_sem, mate)

    def pot_copy(h, g):
        return copy(pot_send, pot_recv.at[mine], pot_sem, (gx, h, g))

    def tot_copy(t, h, g):
        dst = tot_recv.at[gx * crowd + mine]
        return lane_copy(tot_send.at[t, g], dst, tot_sem, t, (t, h, g))

    def back_copy(h, g):
        return copy(back_send.at[g], back_recv.at[mine], back_sem, (gx, h, g))

    def z_copy(index, t):
        return copy(z_send.at[index, t], z_recv.at[index, gx], z_sem, (t, gy, gz), index)

    load_core = pltpu.make_async_copy(core_hbm, core, load_sem.at[0])
    load_vals = pltpu.make_async_copy(colloc_hbm, vals, load_sem.at[1])
    load_place = pltpu.make_async_copy(place_hbm, place, load_sem.at[2])
    spans = [(s, min(DEPTH, total - s)) for s in range(0, total, DEPTH)]
    depth_loads = [
        pltpu.make_async_copy(
            coeffs_hbm.at[pl.ds(s, n)], coeffs.at[pl.ds(s, n)], depth_sem.at[i]
        )
        for i, (s, n) in enumerate(spans)
    ]
    load_core.start()
    load_vals.start()
    depth_loads[0].start()

    barrier = pltpu.get_barrier_semaphore()
    def greet(sem, before):
        for t in range(gx_size):

            @pl.when(gx > t if before else gx < t)
            def _():
                for h, g in across:
                    pl.semaphore_signal(sem, inc=1, device_id=(t, h, g), device_id_type=MESH)

        for h, g in same + [mate[1:]] * (halves - 1):
            i = h * gz_size + g

            @pl.when(i < mine if before else i > mine)
            def _():
                pl.semaphore_signal(sem, inc=1, device_id=(gx, h, g), device_id_type=MESH)

    greet(barrier, False)
    for load in depth_loads[1:]:
        load.start()
    load_place.start()
    below = lax.div(mine, halves) + part
    above = crowd // halves + halves - 2 - below

    @pl.when(gx + below > 0)
    def _():
        pl.semaphore_wait(barrier, gx * len(across) + below)

    greet(ready.at[gx], True)

    def contract(first, last):
        acc = jnp.zeros((points, coeffs.shape[1]), F32)
        for i in range(first, last):
            s, n = spans[i]
            depth_loads[i].wait()
            acc += dot(vals[:, s : s + n], coeffs[s : s + n, :], 1, 0)
        return acc

    load_vals.wait()
    early = len(spans) // 2
    occ = contract(0, early)
    load_core.wait()
    for a in range(gx_size):
        cores[a] = core[:, a * points : (a + 1) * points]
    for d in steps[::2]:

        @pl.when(gx >= d)
        def _():
            lend(gx - d)

    occ += contract(early, len(spans))
    occ = occ.astype(BF16)
    col_occ[own] = occ
    square = jnp.square(occ.astype(F32))
    high = square.astype(BF16)
    low = (square - high.astype(F32)).astype(BF16)
    ones = jnp.ones((8, occ.shape[1]), BF16)
    dens[gx] = (dot(ones, high, 1, 1) + dot(ones, low, 1, 1))[:1]

    @pl.when(above > 0)
    def _():
        pl.semaphore_wait(ready.at[gx], above)

    if halves > 1:
        col_fwd(gy).start()
    for h in sides:
        col_copy(h).start()
    for t in range(gx_size - 1):

        @pl.when(gx > t)
        def _():
            dens_copy(t).start()

        @pl.when((gx > t) & (lax.rem(jnp.abs(gx - t), 2) == 1))
        def _():
            for k in range(halves):
                row_copy(t, k).start()

    for h in sides:
        col_win_copy(h).start()
    for h in range(gy_size):
        stage[h, :, :width] = vals[:, h * width : (h + 1) * width]
        if width < span:
            stage[h, :, width:] = jnp.zeros((points, span - width), BF16)
    lead = part == halves - 1

    @pl.when(lead)
    def _():
        for h in sides:
            cols_copy(h).start()

    own_cols = pltpu.make_async_copy(stage.at[gy], cols.at[gy], load_sem.at[3])
    own_cols.start()
    for t in range(1, gx_size):

        @pl.when(gx < t)
        def _():
            pl.semaphore_wait(ready.at[t], len(across))
            dens_copy(t).start()

        @pl.when((gx < t) & (lax.rem(jnp.abs(gx - t), 2) == 0))
        def _():
            lend(t)
            for k in range(halves):
                row_copy(t, k).start()

    for h, g in same:
        pl.semaphore_signal(known, inc=1, device_id=(gx, h, g), device_id_type=MESH)
    col_win[gy] = vals[:, :lanes]
    load_place.wait()
    for z in range(gx_size):

        @pl.when(jnp.logical_not(keeps(z)))
        def _():
            row_win[z] = jnp.zeros(row_win.shape[1:], BF16)
            core_t[z] = jnp.zeros(core_t.shape[1:], BF16)

        @pl.when((gx != z) & jnp.logical_not(keeps(z)))
        def _():
            row_occ[pl.ds(z * halves, halves)] = jnp.zeros((halves, *row_occ.shape[1:]), BF16)

        @pl.when((gx != z) & jnp.logical_not(kept_by(z)))
        def _():
            tot_recv[pl.ds(z * crowd, crowd)] = jnp.zeros((crowd, *tot_recv.shape[1:]), BF16)

    spread = place[...]
    for k in range(halves):

        @pl.when(part == k)
        def _():
            starts = [a * points + k * half for a in range(gx_size)]
            core_q[...] = jnp.concatenate([core[:, s : s + half] for s in starts], axis=1)

    if sides:
        arrive(col_occ.at[pl.ds(0, len(sides))], col_sem)
    if halves > 1:
        for h in sides:
            col_fwd(h).start()
    if sides:
        arrive(col_win.at[pl.ds(0, len(sides))], col_win_sem)
    wins = dot(spread, col_win[...].reshape(side, lanes), 0, 1)
    win_t[...] = wins.reshape(win_t.shape)
    win_rows = wins.astype(BF16)

    if halves > 1:
        arrive(col_occ.at[pl.ds(0, gy_size)], col_sem, 1)
    for k in range(halves):
        row_occ[gx * halves + k] = col_occ[gy * halves + k, own_rows]
    tight = win_t.shape[1]
    layers = tight // 8

    if planes:
        arrive(dens.at[pl.ds(0, len(planes))], dens_sem)
    density = jnp.concatenate([dens[z] for z in range(gx_size)], axis=1)
    density = jnp.broadcast_to(density, (8, core.shape[1])).astype(BF16)
    potential = dot(density, core[...], 1, 1)[:1]
    pot_send[...] = potential
    if same:
        pl.semaphore_wait(known, len(same))
    for h, g in flat:
        pot_copy(h, g).start()

    def side_occ(k):
        return jnp.concatenate([col_occ[h * halves + k] for h in range(gy_size)], axis=0)

    def line_occ(k):
        return jnp.concatenate([row_occ[z * halves + k] for z in range(gx_size)], axis=0)

    for d in steps:
        z = other(d)

        @pl.when(inside(z))
        def _():
            lane_wait(row_occ.at[pl.ds(z * halves, halves)], row_sem, z)

    gram = sum(dot(side_occ(k), line_occ(k), 1, 1) for k in range(halves))
    mixed = (core_q[...].astype(F32) * gram).astype(BF16)
    block = dot(win_rows, mixed, 1, 0)
    bands = []
    for j in range(layers):
        starts = [g * tight + j * 8 for g in range(gz_size)]
        bands.append(jnp.concatenate([block[at : at + 8] for at in starts], axis=0))
    for z in reversed(range(gx_size)):
        pack = [band[:, z * half : (z + 1) * half] for band in bands]
        pack = jnp.concatenate(pack, axis=1).reshape(tot_send.shape[1:])
        tot_send[z] = pack.astype(BF16)

        @pl.when(keeps(z))
        def _():
            sweep(lambda i: tot_copy(z, *seat(i)).start())

    for h, g in flat:
        tot_copy(gx, h, g).start()
    own_tot = pltpu.make_async_copy(
        tot_send.at[gx, gz], tot_recv.at[gx * crowd + mine], tot_sem.at[1, gx]
    )
    own_tot.start()
    for d in steps:
        z = other(d)

        @pl.when(inside(z))
        def _():
            lane_wait(row_win.at[z], row_win_sem, z)
            lane_wait(core_t.at[z], core_sem, z)

    core_vals = [
        core_t[:, h].reshape(gx_size * half, points).astype(F32) for h in range(gy_size)
    ]
    far_win = dot(spread, row_win[...].reshape(-1, lanes), 0, 1).astype(BF16)
    gram = sum(dot(line_occ(k), side_occ(k), 1, 1) for k in range(halves))
    mixed = (jnp.concatenate(core_vals, axis=1) * gram).astype(BF16)
    back = dot(far_win, mixed, 1, 0)
    back_send[...] = back.reshape(back_send.shape).astype(BF16)
    for h, g in flat:
        back_copy(h, g).start()
    own_back = pltpu.make_async_copy(back_send.at[gz], back_recv.at[mine], back_sem.at[1])
    own_back.start()

    if sides:

        @pl.when(lead)
        def _():
            arrive(cols.at[pl.ds(0, len(sides))], cols_sem)
            if halves > 1:
                for h in sides:
                    cols_fwd(h).start()

    spare = 8 - rows
    reach = z_send.shape[3]
    tail = span - reach

    def spread_out(index, left):
        gap = jnp.zeros((spare, side), F32)
        lines = []
        for a in range(gx_size):
            lines += [left[a * rows : (a + 1) * rows], gap]
        lefts = jnp.concatenate(lines, axis=0).astype(BF16)
        out = dot(lefts, cols[...].reshape(side, span), 1, 0).reshape(gx_size, 8, span)
        line = lax.broadcasted_iota(jnp.int32, (8, tail), 0)
        for a in range(gx_size):
            for j in range(reach // tail):
                block = out[a, :, j * tail : (j + 1) * tail]
                if j * spare < rows:
                    moved = pltpu.roll(out[a, :, reach:], (rows - j * spare) % 8, 0)
                    block = jnp.where(line < rows, block, moved)
                z_send[index, a, :, j * tail : (j + 1) * tail] = block.astype(BF16)
            if reach % tail:
                at = reach // tail * tail
                z_send[index, a, :, at:] = out[a, :, at:reach].astype(BF16)
        for t in range(gx_size):

            @pl.when(gx != t)
            def _():
                z_copy(index, t).start()

    if flat:
        arrive(pot_recv.at[pl.ds(0, len(flat))], pot_sem)
    pot = pot_send[...]
    for h, g in flat:
        pot += pot_recv[h * gz_size + g]
    weighted = (win_t[gz] * pot).astype(BF16).astype(F32)
    own_cols.wait()
    if halves > 1 and sides:

        @pl.when(part == 0)
        def _():
            arrive(cols.at[pl.ds(0, len(sides))], cols_fwd_sem)

    spread_out(0, weighted)

    arrive(back_recv, back_sem)
    for z in range(gx_size):

        @pl.when((gx == z) | kept_by(z))
        def _():
            lane_wait(tot_recv.at[pl.ds(z * crowd, crowd)], tot_sem, z)

    total_of = []
    for i in range(gy_size * halves):
        h, k = divmod(i, halves)
        slots = [
            z * crowd + h * gz_size + g
            for z in range(gx_size)
            for g in range(k, gz_size, halves)
        ]
        total_of.append(sum(tot_recv[slot].astype(F32) for slot in slots))
    owned = [
        jnp.concatenate([one[:, j * half : (j + 1) * half] for one in total_of], axis=1)
        for j in range(layers)
    ]
    owned = jnp.concatenate(owned, axis=0)
    owned += sum(back_recv[i].astype(F32) for i in range(crowd)).reshape(owned.shape)
    spread_out(1, owned)

    if sides:
        leave(col_win.at[pl.ds(0, len(sides))], col_win_sem)

        @pl.when(lead)
        def _():
            leave(cols.at[pl.ds(0, len(sides))], cols_sem)
            if halves > 1:
                leave(cols.at[pl.ds(0, len(sides))], cols_fwd_sem)

    if planes:
        leave(dens.at[pl.ds(0, len(planes))], dens_sem)
    leave(col_occ.at[pl.ds(0, len(sides) + gy_size * (halves - 1))], col_sem)
    leave(pot_recv.at[pl.ds(0, len(flat))], pot_sem)
    leave(back_recv.at[pl.ds(0, len(flat))], back_sem)
    lane_leave(tot_recv.at[pl.ds(0, len(flat))], tot_sem, gx)
    for d in steps:
        t, z = keeper(d), other(d)

        @pl.when(inside(t))
        def _():
            lane_leave(row_occ.at[pl.ds(0, halves)], row_sem, t)
            lane_leave(row_win.at[0], row_win_sem, t)
            lane_leave(core_t.at[0], core_sem, t)

        @pl.when(inside(z))
        def _():
            lane_leave(tot_recv.at[pl.ds(0, crowd)], tot_sem, z)


    for index in range(2):
        if planes:
            arrive(z_recv.at[index, pl.ds(0, len(planes))], z_sem, index)
        acc = z_send[index, gx].astype(F32)
        for z in planes:
            acc += z_recv[index, z].astype(F32)
        out_ref[index, :, :reach] = acc[:rows]
        for r in range(rows):
            j, k = divmod(r, spare)
            line = acc[rows + k : rows + k + 1, j * tail : j * tail + width - reach]
            out_ref[index, r : r + 1, reach:] = line

    if planes:
        leave(z_recv.at[:, pl.ds(0, len(planes))], z_sem)


def local(colloc, occ_coeffs, core):
    points, total = colloc.shape
    gx_size = lax.axis_size("gx")
    gy_size = lax.axis_size("gy")
    gz_size = lax.axis_size("gz")
    occupied = occ_coeffs.shape[1]
    rows = W // (gx_size * gz_size)
    width = total // gy_size
    row_count, flat = core.shape[0], core.shape[2]
    lanes = up(W, LANES)
    side = gy_size * points
    span = up(width, LANES)
    halves = 2 if gz_size % 2 == 0 else 1
    half = points // halves
    tiles = span // LANES
    spare = 8 - rows
    tail = max(t for t in range(1, tiles) if (tiles - t) // t * spare >= rows)
    reach = span - tail * LANES

    used = gx_size * rows
    tight = up(used, 8)
    place = np.zeros((lanes, gz_size, tight), np.float32)
    for a in range(gx_size):
        for g in range(gz_size):
            for k in range(rows):
                place[(a * gz_size + g) * rows + k, g, a * rows + k] = 1
    place = jnp.asarray(place.reshape(lanes, gz_size * tight), BF16)

    dims = (gx_size, gy_size, gz_size, rows, width)
    dma = pltpu.SemaphoreType.DMA
    vmem = pltpu.VMEM
    result = pl.pallas_call(
        functools.partial(kernel, dims),
        out_shape=pltpu.VMEM((2, rows, width), F32),
        in_specs=[pl.BlockSpec(memory_space=pltpu.HBM)] * 4,
        out_specs=pl.BlockSpec(memory_space=pltpu.VMEM),
        scratch_shapes=[
            vmem((points, total), BF16),
            vmem((total, occupied), BF16),
            vmem((row_count, flat), BF16),
            vmem(place.shape, BF16),
            vmem((row_count, gx_size * half), BF16),
            vmem((gx_size, row_count, points), BF16),
            vmem((gx_size, gy_size, half, points), BF16),
            vmem((gx_size, half, lanes), BF16),
            vmem((gx_size * halves, half, occupied), BF16),
            vmem((gy_size * halves, points, occupied), BF16),
            vmem((gy_size, points, lanes), BF16),
            vmem((gz_size, tight, side), F32),
            vmem((gx_size, 1, points), F32),
            vmem((gy_size, points, span), BF16),
            vmem((gy_size, points, span), BF16),
            vmem((1, side), F32),
            vmem((gy_size * gz_size, 1, side), F32),
            vmem((gx_size, gz_size, 8, tight // 8 * half), BF16),
            vmem((gx_size * gy_size * gz_size, 8, tight // 8 * half), BF16),
            vmem((gz_size, tight // 8, 8, side), BF16),
            vmem((gy_size * gz_size, tight // 8, 8, side), BF16),
            vmem((2, gx_size, 8, reach), BF16),
            vmem((2, gx_size, 8, reach), BF16),
            dma((4,)),
            dma((-(-total // DEPTH),)),
            pltpu.SemaphoreType.REGULAR((gx_size,)),
            pltpu.SemaphoreType.REGULAR,
            dma((2, gx_size)),
            dma((2, gx_size)),
            dma((2, gx_size)),
            dma((3,)),
            dma((2,)),
            dma((2,)),
            dma((2,)),
            dma((2,)),
            dma((2,)),
            dma((2, gx_size)),
            dma((2,)),
            dma((3,)),
        ],
        compiler_params=pltpu.CompilerParams(
            collective_id=0, has_side_effects=True, vmem_limit_bytes=60 * 1024 * 1024
        ),
    )(colloc, occ_coeffs, core.reshape(row_count, flat), place)
    return result[0], result[1]


def solution(mesh):
    in_specs = (P(("gx", "gy"), None), P(None, "gz"), P("gx", "gy", None))
    out_specs = (P(("gx", "gz"), "gy"), P(("gx", "gz"), "gy"))
    return jax.shard_map(local, mesh=mesh, in_specs=in_specs, out_specs=out_specs, check_vma=False)
```

```python
import functools

import jax
import jax.numpy as jnp
import numpy as np
from jax import lax
from jax.experimental import pallas as pl
from jax.experimental.pallas import tpu as pltpu
from jax.sharding import PartitionSpec as P

W = 96
LANES = 128
DEPTH = 1024
MESH = pl.DeviceIdType.MESH
F32 = jnp.float32
BF16 = jnp.bfloat16


def up(value, step):
    return -(-value // step) * step


def dot(left, right, left_dim, right_dim):
    return lax.dot_general(
        left, right, (((left_dim,), (right_dim,)), ((), ())), preferred_element_type=F32
    )


def kernel(
    dims,
    colloc_hbm,
    coeffs_hbm,
    core_hbm,
    place_hbm,
    out_ref,
    vals,
    coeffs,
    core,
    place,
    core_q,
    cores,
    core_t,
    row_win,
    row_occ,
    col_occ,
    col_win,
    win_t,
    dens,
    stage,
    cols,
    pot_send,
    pot_recv,
    tot_send,
    tot_recv,
    back_send,
    back_recv,
    z_send,
    z_recv,
    load_sem,
    depth_sem,
    ready,
    known,
    row_sem,
    core_sem,
    row_win_sem,
    col_sem,
    col_win_sem,
    dens_sem,
    cols_sem,
    cols_fwd_sem,
    pot_sem,
    tot_sem,
    back_sem,
    z_sem,
):
    gx_size, gy_size, gz_size, rows, width = dims
    gx, gy, gz = lax.axis_index("gx"), lax.axis_index("gy"), lax.axis_index("gz")
    points, total = vals.shape
    lanes = col_win.shape[2]
    crowd = gy_size * gz_size
    halves = 2 if gz_size % 2 == 0 else 1
    half = points // halves
    base = gz - lax.rem(gz, halves)
    span = cols.shape[2]
    side = gy_size * points
    part = lax.rem(gz, halves)

    def turn(pos, step, size):
        if size & (size - 1):
            return lax.rem(pos + step, size) if step else pos
        bit = 1
        while bit <= step:
            if step & bit:
                pos = pos + bit * (1 - 2 * lax.rem(lax.div(pos, bit), 2))
            bit *= 2
        return pos

    planes = [turn(gx, d, gx_size) for d in range(1, gx_size)]
    sides = [turn(gy, d, gy_size) for d in range(1, gy_size)]
    flat = [
        (turn(gy, dy, gy_size), turn(gz, dz, gz_size))
        for dy in range(gy_size)
        for dz in range(gz_size)
        if dy or dz
    ]
    across = [(gy, base + k) for k in range(halves)] + [(h, gz) for h in sides]
    mine = gy * gz_size + gz
    own = gy * halves + part
    mate = (gx, gy, base + halves - 1 - part)
    same = [
        (turn(gy, dy, gy_size), turn(gz, dz, gz_size))
        for dy in range(gy_size)
        for dz in range(0, gz_size, halves)
        if dy or dz
    ]

    def copy(src, dst, sems, target, slot=0):
        return pltpu.make_async_remote_copy(
            src_ref=src,
            dst_ref=dst,
            send_sem=sems.at[0],
            recv_sem=sems.at[1 + slot],
            device_id=target,
            device_id_type=MESH,
        )

    def arrive(ref, sems, slot=0):
        copy(ref, ref, sems, mate, slot).wait_recv()

    def leave(ref, sems):
        copy(ref, ref, sems, mate).wait_send()

    def lane_copy(src, dst, sems, t, target):
        return pltpu.make_async_remote_copy(
            src_ref=src,
            dst_ref=dst,
            send_sem=sems.at[0, t],
            recv_sem=sems.at[1, gx],
            device_id=target,
            device_id_type=MESH,
        )

    def lane_wait(ref, sems, z):
        pltpu.make_async_remote_copy(
            src_ref=ref,
            dst_ref=ref,
            send_sem=sems.at[0, z],
            recv_sem=sems.at[1, z],
            device_id=mate,
            device_id_type=MESH,
        ).wait_recv()

    def lane_leave(ref, sems, t):
        pltpu.make_async_remote_copy(
            src_ref=ref,
            dst_ref=ref,
            send_sem=sems.at[0, t],
            recv_sem=sems.at[1, t],
            device_id=mate,
            device_id_type=MESH,
        ).wait_send()

    steps = range(1, gx_size)

    def other(d):
        return gx + d if d % 2 else gx - d

    def keeper(d):
        return gx - d if d % 2 else gx + d

    def inside(t):
        return (t >= 0) & (t < gx_size)

    def keeps(z):
        gap = z - gx
        odd = lax.rem(jnp.abs(gap), 2)
        return ((gap > 0) & (odd == 1)) | ((gap < 0) & (odd == 0))

    def kept_by(z):
        gap = gx - z
        odd = lax.rem(jnp.abs(gap), 2)
        return ((gap > 0) & (odd == 1)) | ((gap < 0) & (odd == 0))

    def seat(i):
        return lax.div(i, gz_size), lax.rem(i, gz_size)

    def sweep(body):
        if crowd <= 16:
            for i in range(crowd):
                body(jnp.int32(i))
        else:
            lax.fori_loop(0, crowd, lambda i, c: (body(i), c)[1], 0)

    own_rows = pl.ds(pl.multiple_of(part * half, half), half)

    def col_win_copy(h):
        return copy(vals.at[:, pl.ds(0, lanes)], col_win.at[gy], col_win_sem, (gx, h, gz))

    def dens_copy(t):
        some = dens.at[gx]
        return copy(some, some, dens_sem, (t, gy, gz))

    def row_copy(t, k):
        src = col_occ.at[own, pl.ds(k * half, half)]
        return lane_copy(src, row_occ.at[gx * halves + part], row_sem, t, (t, gy, base + k))

    def core_copy(t, h):
        src = cores.at[t, pl.ds(pl.multiple_of(h * points + part * half, half), half)]
        return lane_copy(src, core_t.at[gx, gy], core_sem, t, (t, h, gz))

    def row_win_copy(t):
        src = vals.at[own_rows, pl.ds(0, lanes)]
        return lane_copy(src, row_win.at[gx], row_win_sem, t, (t, gy, gz))

    def lend(t):
        for h in range(gy_size):
            core_copy(t, h).start()

    def col_copy(h):
        some = col_occ.at[own]
        return copy(some, some, col_sem, (gx, h, gz))

    def col_fwd(h):
        some = col_occ.at[h * halves + part]
        return copy(some, some, col_sem, mate, 1)

    def cols_copy(h):
        return copy(stage.at[h], cols.at[gy], cols_sem, (gx, h, gz))

    def cols_fwd(h):
        some = cols.at[h]
        return copy(some, some, cols_fwd_sem, mate)

    def pot_copy(h, g):
        return copy(pot_send, pot_recv.at[mine], pot_sem, (gx, h, g))

    def tot_copy(t, h, g):
        dst = tot_recv.at[gx * crowd + mine]
        return lane_copy(tot_send.at[t, g], dst, tot_sem, t, (t, h, g))

    def back_copy(h, g):
        return copy(back_send.at[g], back_recv.at[mine], back_sem, (gx, h, g))

    def z_copy(index, t):
        return copy(z_send.at[index, t], z_recv.at[index, gx], z_sem, (t, gy, gz), index)

    load_core = pltpu.make_async_copy(core_hbm, core, load_sem.at[0])
    load_vals = pltpu.make_async_copy(colloc_hbm, vals, load_sem.at[1])
    load_place = pltpu.make_async_copy(place_hbm, place, load_sem.at[2])
    spans = [(s, min(DEPTH, total - s)) for s in range(0, total, DEPTH)]
    depth_loads = [
        pltpu.make_async_copy(
            coeffs_hbm.at[pl.ds(s, n)], coeffs.at[pl.ds(s, n)], depth_sem.at[i]
        )
        for i, (s, n) in enumerate(spans)
    ]
    load_core.start()
    load_vals.start()
    depth_loads[0].start()

    barrier = pltpu.get_barrier_semaphore()
    def greet(sem, before):
        for t in range(gx_size):

            @pl.when(gx > t if before else gx < t)
            def _():
                for h, g in across:
                    pl.semaphore_signal(sem, inc=1, device_id=(t, h, g), device_id_type=MESH)

        for h, g in same + [mate[1:]] * (halves - 1):
            i = h * gz_size + g

            @pl.when(i < mine if before else i > mine)
            def _():
                pl.semaphore_signal(sem, inc=1, device_id=(gx, h, g), device_id_type=MESH)

    greet(barrier, False)
    for load in depth_loads[1:]:
        load.start()
    load_place.start()
    below = lax.div(mine, halves) + part
    above = crowd // halves + halves - 2 - below

    @pl.when(gx + below > 0)
    def _():
        pl.semaphore_wait(barrier, gx * len(across) + below)

    greet(ready.at[gx], True)

    def contract(first, last):
        acc = jnp.zeros((points, coeffs.shape[1]), F32)
        for i in range(first, last):
            s, n = spans[i]
            depth_loads[i].wait()
            acc += dot(vals[:, s : s + n], coeffs[s : s + n, :], 1, 0)
        return acc

    load_core.wait()
    for a in range(gx_size):
        cores[a] = core[:, a * points : (a + 1) * points]
    for d in steps[::2]:

        @pl.when(gx >= d)
        def _():
            lend(gx - d)

    load_vals.wait()
    for d in steps[::2]:

        @pl.when(gx >= d)
        def _():
            row_win_copy(gx - d).start()

    occ = contract(0, len(spans))
    occ = occ.astype(BF16)
    col_occ[own] = occ
    @pl.when(above > 0)
    def _():
        pl.semaphore_wait(ready.at[gx], above)

    if halves > 1:
        col_fwd(gy).start()
    for h in sides:
        col_copy(h).start()
    square = jnp.square(occ.astype(F32))
    high = square.astype(BF16)
    low = (square - high.astype(F32)).astype(BF16)
    ones = jnp.ones((8, occ.shape[1]), BF16)
    dens[gx] = (dot(ones, high, 1, 1) + dot(ones, low, 1, 1))[:1]

    for t in range(gx_size - 1):

        @pl.when(gx > t)
        def _():
            dens_copy(t).start()

        @pl.when((gx > t) & (lax.rem(jnp.abs(gx - t), 2) == 1))
        def _():
            for k in range(halves):
                row_copy(t, k).start()

    for h in sides:
        col_win_copy(h).start()
    for h in range(gy_size):
        stage[h, :, :width] = vals[:, h * width : (h + 1) * width]
        if width < span:
            stage[h, :, width:] = jnp.zeros((points, span - width), BF16)
    lead = part == halves - 1

    @pl.when(lead)
    def _():
        for h in sides:
            cols_copy(h).start()

    own_cols = pltpu.make_async_copy(stage.at[gy], cols.at[gy], load_sem.at[3])
    own_cols.start()
    for t in range(1, gx_size):

        @pl.when(gx < t)
        def _():
            pl.semaphore_wait(ready.at[t], len(across))
            dens_copy(t).start()

        @pl.when((gx < t) & (lax.rem(jnp.abs(gx - t), 2) == 0))
        def _():
            lend(t)
            row_win_copy(t).start()
            for k in range(halves):
                row_copy(t, k).start()

    for h, g in same:
        pl.semaphore_signal(known, inc=1, device_id=(gx, h, g), device_id_type=MESH)
    col_win[gy] = vals[:, :lanes]
    load_place.wait()
    for z in range(gx_size):

        @pl.when(jnp.logical_not(keeps(z)))
        def _():
            row_win[z] = jnp.zeros(row_win.shape[1:], BF16)
            core_t[z] = jnp.zeros(core_t.shape[1:], BF16)

        @pl.when((gx != z) & jnp.logical_not(keeps(z)))
        def _():
            row_occ[pl.ds(z * halves, halves)] = jnp.zeros((halves, *row_occ.shape[1:]), BF16)

        @pl.when((gx != z) & jnp.logical_not(kept_by(z)))
        def _():
            tot_recv[pl.ds(z * crowd, crowd)] = jnp.zeros((crowd, *tot_recv.shape[1:]), BF16)

    spread = place[...]
    for k in range(halves):

        @pl.when(part == k)
        def _():
            starts = [a * points + k * half for a in range(gx_size)]
            core_q[...] = jnp.concatenate([core[:, s : s + half] for s in starts], axis=1)

    if sides:
        arrive(col_occ.at[pl.ds(0, len(sides))], col_sem)
    if halves > 1:
        for h in sides:
            col_fwd(h).start()
    if sides:
        arrive(col_win.at[pl.ds(0, len(sides))], col_win_sem)
    wins = dot(spread, col_win[...].reshape(side, lanes), 0, 1)
    win_t[...] = wins.reshape(win_t.shape)
    win_rows = wins.astype(BF16)

    if halves > 1:
        arrive(col_occ.at[pl.ds(0, gy_size)], col_sem, 1)
    for k in range(halves):
        row_occ[gx * halves + k] = col_occ[gy * halves + k, own_rows]
    tight = win_t.shape[1]
    layers = tight // 8

    if planes:
        arrive(dens.at[pl.ds(0, len(planes))], dens_sem)
    density = jnp.concatenate([dens[z] for z in range(gx_size)], axis=1)
    density = jnp.broadcast_to(density, (8, core.shape[1])).astype(BF16)
    potential = dot(density, core[...], 1, 1)[:1]
    pot_send[...] = potential
    if same:
        pl.semaphore_wait(known, len(same))
    for h, g in flat:
        pot_copy(h, g).start()

    def side_occ(k):
        return jnp.concatenate([col_occ[h * halves + k] for h in range(gy_size)], axis=0)

    def line_occ(k):
        return jnp.concatenate([row_occ[z * halves + k] for z in range(gx_size)], axis=0)

    for d in steps:
        z = other(d)

        @pl.when(inside(z))
        def _():
            lane_wait(row_occ.at[pl.ds(z * halves, halves)], row_sem, z)

    gram = sum(dot(side_occ(k), line_occ(k), 1, 1) for k in range(halves))
    mixed = (core_q[...].astype(F32) * gram).astype(BF16)
    block = dot(win_rows, mixed, 1, 0)
    bands = []
    for j in range(layers):
        starts = [g * tight + j * 8 for g in range(gz_size)]
        bands.append(jnp.concatenate([block[at : at + 8] for at in starts], axis=0))
    for z in reversed(range(gx_size)):
        pack = [band[:, z * half : (z + 1) * half] for band in bands]
        pack = jnp.concatenate(pack, axis=1).reshape(tot_send.shape[1:])
        tot_send[z] = pack.astype(BF16)

        @pl.when(keeps(z))
        def _():
            sweep(lambda i: tot_copy(z, *seat(i)).start())

    for h, g in flat:
        tot_copy(gx, h, g).start()
    own_tot = pltpu.make_async_copy(
        tot_send.at[gx, gz], tot_recv.at[gx * crowd + mine], tot_sem.at[1, gx]
    )
    own_tot.start()
    for d in steps:
        z = other(d)

        @pl.when(inside(z))
        def _():
            lane_wait(row_win.at[z], row_win_sem, z)
            lane_wait(core_t.at[z], core_sem, z)

    core_vals = [
        core_t[:, h].reshape(gx_size * half, points).astype(F32) for h in range(gy_size)
    ]
    far_win = dot(spread, row_win[...].reshape(-1, lanes), 0, 1).astype(BF16)
    gram = sum(dot(line_occ(k), side_occ(k), 1, 1) for k in range(halves))
    mixed = (jnp.concatenate(core_vals, axis=1) * gram).astype(BF16)
    back = dot(far_win, mixed, 1, 0)
    back_send[...] = back.reshape(back_send.shape).astype(BF16)
    for h, g in flat:
        back_copy(h, g).start()
    own_back = pltpu.make_async_copy(back_send.at[gz], back_recv.at[mine], back_sem.at[1])
    own_back.start()

    if sides:

        @pl.when(lead)
        def _():
            arrive(cols.at[pl.ds(0, len(sides))], cols_sem)
            if halves > 1:
                for h in sides:
                    cols_fwd(h).start()

    spare = 8 - rows
    reach = z_send.shape[3]
    tail = span - reach

    def spread_out(index, left):
        gap = jnp.zeros((spare, side), F32)
        lines = []
        for a in range(gx_size):
            lines += [left[a * rows : (a + 1) * rows], gap]
        lefts = jnp.concatenate(lines, axis=0).astype(BF16)
        out = dot(lefts, cols[...].reshape(side, span), 1, 0).reshape(gx_size, 8, span)
        line = lax.broadcasted_iota(jnp.int32, (8, tail), 0)
        for a in range(gx_size):
            for j in range(reach // tail):
                block = out[a, :, j * tail : (j + 1) * tail]
                if j * spare < rows:
                    moved = pltpu.roll(out[a, :, reach:], (rows - j * spare) % 8, 0)
                    block = jnp.where(line < rows, block, moved)
                z_send[index, a, :, j * tail : (j + 1) * tail] = block.astype(BF16)
            if reach % tail:
                at = reach // tail * tail
                z_send[index, a, :, at:] = out[a, :, at:reach].astype(BF16)
        for t in range(gx_size):

            @pl.when(gx != t)
            def _():
                z_copy(index, t).start()

    if flat:
        arrive(pot_recv.at[pl.ds(0, len(flat))], pot_sem)
    pot = pot_send[...]
    for h, g in flat:
        pot += pot_recv[h * gz_size + g]
    weighted = (win_t[gz] * pot).astype(BF16).astype(F32)
    own_cols.wait()
    if halves > 1 and sides:

        @pl.when(part == 0)
        def _():
            arrive(cols.at[pl.ds(0, len(sides))], cols_fwd_sem)

    spread_out(0, weighted)

    arrive(back_recv, back_sem)
    for z in range(gx_size):

        @pl.when((gx == z) | kept_by(z))
        def _():
            lane_wait(tot_recv.at[pl.ds(z * crowd, crowd)], tot_sem, z)

    total_of = []
    for i in range(gy_size * halves):
        h, k = divmod(i, halves)
        slots = [
            z * crowd + h * gz_size + g
            for z in range(gx_size)
            for g in range(k, gz_size, halves)
        ]
        total_of.append(sum(tot_recv[slot].astype(F32) for slot in slots))
    owned = [
        jnp.concatenate([one[:, j * half : (j + 1) * half] for one in total_of], axis=1)
        for j in range(layers)
    ]
    owned = jnp.concatenate(owned, axis=0)
    owned += sum(back_recv[i].astype(F32) for i in range(crowd)).reshape(owned.shape)
    spread_out(1, owned)

    if sides:
        leave(col_win.at[pl.ds(0, len(sides))], col_win_sem)

        @pl.when(lead)
        def _():
            leave(cols.at[pl.ds(0, len(sides))], cols_sem)
            if halves > 1:
                leave(cols.at[pl.ds(0, len(sides))], cols_fwd_sem)

    if planes:
        leave(dens.at[pl.ds(0, len(planes))], dens_sem)
    leave(col_occ.at[pl.ds(0, len(sides) + gy_size * (halves - 1))], col_sem)
    leave(pot_recv.at[pl.ds(0, len(flat))], pot_sem)
    leave(back_recv.at[pl.ds(0, len(flat))], back_sem)
    lane_leave(tot_recv.at[pl.ds(0, len(flat))], tot_sem, gx)
    for d in steps:
        t, z = keeper(d), other(d)

        @pl.when(inside(t))
        def _():
            lane_leave(row_occ.at[pl.ds(0, halves)], row_sem, t)
            lane_leave(row_win.at[0], row_win_sem, t)
            lane_leave(core_t.at[0], core_sem, t)

        @pl.when(inside(z))
        def _():
            lane_leave(tot_recv.at[pl.ds(0, crowd)], tot_sem, z)


    for index in range(2):
        if planes:
            arrive(z_recv.at[index, pl.ds(0, len(planes))], z_sem, index)
        acc = z_send[index, gx].astype(F32)
        for z in planes:
            acc += z_recv[index, z].astype(F32)
        out_ref[index, :, :reach] = acc[:rows]
        for r in range(rows):
            j, k = divmod(r, spare)
            line = acc[rows + k : rows + k + 1, j * tail : j * tail + width - reach]
            out_ref[index, r : r + 1, reach:] = line

    if planes:
        leave(z_recv.at[:, pl.ds(0, len(planes))], z_sem)


def local(colloc, occ_coeffs, core):
    points, total = colloc.shape
    gx_size = lax.axis_size("gx")
    gy_size = lax.axis_size("gy")
    gz_size = lax.axis_size("gz")
    occupied = occ_coeffs.shape[1]
    rows = W // (gx_size * gz_size)
    width = total // gy_size
    row_count, flat = core.shape[0], core.shape[2]
    lanes = up(W, LANES)
    side = gy_size * points
    span = up(width, LANES)
    halves = 2 if gz_size % 2 == 0 else 1
    half = points // halves
    tiles = span // LANES
    spare = 8 - rows
    tail = max(t for t in range(1, tiles) if (tiles - t) // t * spare >= rows)
    reach = span - tail * LANES

    used = gx_size * rows
    tight = up(used, 8)
    place = np.zeros((lanes, gz_size, tight), np.float32)
    for a in range(gx_size):
        for g in range(gz_size):
            for k in range(rows):
                place[(a * gz_size + g) * rows + k, g, a * rows + k] = 1
    place = jnp.asarray(place.reshape(lanes, gz_size * tight), BF16)

    dims = (gx_size, gy_size, gz_size, rows, width)
    dma = pltpu.SemaphoreType.DMA
    vmem = pltpu.VMEM
    result = pl.pallas_call(
        functools.partial(kernel, dims),
        out_shape=pltpu.VMEM((2, rows, width), F32),
        in_specs=[pl.BlockSpec(memory_space=pltpu.HBM)] * 4,
        out_specs=pl.BlockSpec(memory_space=pltpu.VMEM),
        scratch_shapes=[
            vmem((points, total), BF16),
            vmem((total, occupied), BF16),
            vmem((row_count, flat), BF16),
            vmem(place.shape, BF16),
            vmem((row_count, gx_size * half), BF16),
            vmem((gx_size, row_count, points), BF16),
            vmem((gx_size, gy_size, half, points), BF16),
            vmem((gx_size, half, lanes), BF16),
            vmem((gx_size * halves, half, occupied), BF16),
            vmem((gy_size * halves, points, occupied), BF16),
            vmem((gy_size, points, lanes), BF16),
            vmem((gz_size, tight, side), F32),
            vmem((gx_size, 1, points), F32),
            vmem((gy_size, points, span), BF16),
            vmem((gy_size, points, span), BF16),
            vmem((1, side), F32),
            vmem((gy_size * gz_size, 1, side), F32),
            vmem((gx_size, gz_size, 8, tight // 8 * half), BF16),
            vmem((gx_size * gy_size * gz_size, 8, tight // 8 * half), BF16),
            vmem((gz_size, tight // 8, 8, side), BF16),
            vmem((gy_size * gz_size, tight // 8, 8, side), BF16),
            vmem((2, gx_size, 8, reach), BF16),
            vmem((2, gx_size, 8, reach), BF16),
            dma((4,)),
            dma((-(-total // DEPTH),)),
            pltpu.SemaphoreType.REGULAR((gx_size,)),
            pltpu.SemaphoreType.REGULAR,
            dma((2, gx_size)),
            dma((2, gx_size)),
            dma((2, gx_size)),
            dma((3,)),
            dma((2,)),
            dma((2,)),
            dma((2,)),
            dma((2,)),
            dma((2,)),
            dma((2, gx_size)),
            dma((2,)),
            dma((3,)),
        ],
        compiler_params=pltpu.CompilerParams(
            collective_id=0, has_side_effects=True, vmem_limit_bytes=60 * 1024 * 1024
        ),
    )(colloc, occ_coeffs, core.reshape(row_count, flat), place)
    return result[0], result[1]


def solution(mesh):
    in_specs = (P(("gx", "gy"), None), P(None, "gz"), P("gx", "gy", None))
    out_specs = (P(("gx", "gz"), "gy"), P(("gx", "gz"), "gy"))
    return jax.shard_map(local, mesh=mesh, in_specs=in_specs, out_specs=out_specs, check_vma=False)
```

```python
import functools

import jax
import jax.numpy as jnp
import numpy as np
from jax import lax
from jax.experimental import pallas as pl
from jax.experimental.pallas import tpu as pltpu
from jax.sharding import PartitionSpec as P

W = 96
LANES = 128
DEPTH = 1024
MESH = pl.DeviceIdType.MESH
F32 = jnp.float32
BF16 = jnp.bfloat16


def up(value, step):
    return -(-value // step) * step


def dot(left, right, left_dim, right_dim):
    return lax.dot_general(
        left, right, (((left_dim,), (right_dim,)), ((), ())), preferred_element_type=F32
    )


def kernel(
    dims,
    colloc_hbm,
    coeffs_hbm,
    core_hbm,
    place_hbm,
    out_ref,
    vals,
    coeffs,
    core,
    place,
    core_q,
    cores,
    core_t,
    row_win,
    row_occ,
    col_occ,
    col_win,
    win_t,
    dens,
    stage,
    cols,
    pot_send,
    pot_recv,
    tot_send,
    tot_recv,
    back_send,
    back_recv,
    z_send,
    z_recv,
    load_sem,
    depth_sem,
    ready,
    known,
    row_sem,
    core_sem,
    row_win_sem,
    col_sem,
    col_win_sem,
    dens_sem,
    cols_sem,
    cols_fwd_sem,
    pot_sem,
    tot_sem,
    back_sem,
    z_sem,
):
    gx_size, gy_size, gz_size, rows, width = dims
    gx, gy, gz = lax.axis_index("gx"), lax.axis_index("gy"), lax.axis_index("gz")
    points, total = vals.shape
    lanes = col_win.shape[2]
    crowd = gy_size * gz_size
    halves = 2 if gz_size % 2 == 0 else 1
    half = points // halves
    base = gz - lax.rem(gz, halves)
    span = cols.shape[2]
    side = gy_size * points
    part = lax.rem(gz, halves)

    def turn(pos, step, size):
        if size & (size - 1):
            return lax.rem(pos + step, size) if step else pos
        bit = 1
        while bit <= step:
            if step & bit:
                pos = pos + bit * (1 - 2 * lax.rem(lax.div(pos, bit), 2))
            bit *= 2
        return pos

    planes = [turn(gx, d, gx_size) for d in range(1, gx_size)]
    sides = [turn(gy, d, gy_size) for d in range(1, gy_size)]
    flat = [
        (turn(gy, dy, gy_size), turn(gz, dz, gz_size))
        for dy in range(gy_size)
        for dz in range(gz_size)
        if dy or dz
    ]
    across = [(gy, base + k) for k in range(halves)] + [(h, gz) for h in sides]
    mine = gy * gz_size + gz
    own = gy * halves + part
    mate = (gx, gy, base + halves - 1 - part)
    same = [
        (turn(gy, dy, gy_size), turn(gz, dz, gz_size))
        for dy in range(gy_size)
        for dz in range(0, gz_size, halves)
        if dy or dz
    ]

    def copy(src, dst, sems, target, slot=0):
        return pltpu.make_async_remote_copy(
            src_ref=src,
            dst_ref=dst,
            send_sem=sems.at[0],
            recv_sem=sems.at[1 + slot],
            device_id=target,
            device_id_type=MESH,
        )

    def arrive(ref, sems, slot=0):
        copy(ref, ref, sems, mate, slot).wait_recv()

    def leave(ref, sems):
        copy(ref, ref, sems, mate).wait_send()

    def lane_copy(src, dst, sems, t, target):
        return pltpu.make_async_remote_copy(
            src_ref=src,
            dst_ref=dst,
            send_sem=sems.at[0, t],
            recv_sem=sems.at[1, gx],
            device_id=target,
            device_id_type=MESH,
        )

    def lane_wait(ref, sems, z):
        pltpu.make_async_remote_copy(
            src_ref=ref,
            dst_ref=ref,
            send_sem=sems.at[0, z],
            recv_sem=sems.at[1, z],
            device_id=mate,
            device_id_type=MESH,
        ).wait_recv()

    def lane_leave(ref, sems, t):
        pltpu.make_async_remote_copy(
            src_ref=ref,
            dst_ref=ref,
            send_sem=sems.at[0, t],
            recv_sem=sems.at[1, t],
            device_id=mate,
            device_id_type=MESH,
        ).wait_send()

    steps = range(1, gx_size)

    def other(d):
        return gx + d if d % 2 else gx - d

    def keeper(d):
        return gx - d if d % 2 else gx + d

    def inside(t):
        return (t >= 0) & (t < gx_size)

    def keeps(z):
        gap = z - gx
        odd = lax.rem(jnp.abs(gap), 2)
        return ((gap > 0) & (odd == 1)) | ((gap < 0) & (odd == 0))

    def kept_by(z):
        gap = gx - z
        odd = lax.rem(jnp.abs(gap), 2)
        return ((gap > 0) & (odd == 1)) | ((gap < 0) & (odd == 0))

    def seat(i):
        return lax.div(i, gz_size), lax.rem(i, gz_size)

    def sweep(body):
        if crowd <= 16:
            for i in range(crowd):
                body(jnp.int32(i))
        else:
            lax.fori_loop(0, crowd, lambda i, c: (body(i), c)[1], 0)

    own_rows = pl.ds(pl.multiple_of(part * half, half), half)

    def col_win_copy(h):
        return copy(vals.at[:, pl.ds(0, lanes)], col_win.at[gy], col_win_sem, (gx, h, gz))

    def dens_copy(t):
        some = dens.at[gx]
        return copy(some, some, dens_sem, (t, gy, gz))

    def row_copy(t, k):
        src = col_occ.at[own, pl.ds(k * half, half)]
        return lane_copy(src, row_occ.at[gx * halves + part], row_sem, t, (t, gy, base + k))

    def core_copy(t, h):
        src = cores.at[t, pl.ds(pl.multiple_of(h * points + part * half, half), half)]
        return lane_copy(src, core_t.at[gx, gy], core_sem, t, (t, h, gz))

    def row_win_copy(t):
        src = vals.at[own_rows, pl.ds(0, lanes)]
        return lane_copy(src, row_win.at[gx], row_win_sem, t, (t, gy, gz))

    def lend(t):
        for h in range(gy_size):
            core_copy(t, h).start()

    def col_copy(h):
        some = col_occ.at[own]
        return copy(some, some, col_sem, (gx, h, gz))

    def col_fwd(h):
        some = col_occ.at[h * halves + part]
        return copy(some, some, col_sem, mate, 1)

    def cols_copy(h):
        return copy(stage.at[h], cols.at[gy], cols_sem, (gx, h, gz))

    def cols_fwd(h):
        some = cols.at[h]
        return copy(some, some, cols_fwd_sem, mate)

    def pot_copy(h, g):
        return copy(pot_send, pot_recv.at[mine], pot_sem, (gx, h, g))

    def tot_copy(t, h, g):
        dst = tot_recv.at[gx * crowd + mine]
        return lane_copy(tot_send.at[t, g], dst, tot_sem, t, (t, h, g))

    def back_copy(h, g):
        return copy(back_send.at[g], back_recv.at[mine], back_sem, (gx, h, g))

    def z_copy(index, t):
        return copy(z_send.at[index, t], z_recv.at[index, gx], z_sem, (t, gy, gz), index)

    load_core = pltpu.make_async_copy(core_hbm, core, load_sem.at[0])
    load_vals = pltpu.make_async_copy(colloc_hbm, vals, load_sem.at[1])
    load_place = pltpu.make_async_copy(place_hbm, place, load_sem.at[2])
    spans = [(s, min(DEPTH, total - s)) for s in range(0, total, DEPTH)]
    depth_loads = [
        pltpu.make_async_copy(
            coeffs_hbm.at[pl.ds(s, n)], coeffs.at[pl.ds(s, n)], depth_sem.at[i]
        )
        for i, (s, n) in enumerate(spans)
    ]
    load_core.start()
    load_vals.start()
    depth_loads[0].start()

    barrier = pltpu.get_barrier_semaphore()
    def greet(sem, before):
        for t in range(gx_size):

            @pl.when(gx > t if before else gx < t)
            def _():
                for h, g in across:
                    pl.semaphore_signal(sem, inc=1, device_id=(t, h, g), device_id_type=MESH)

        for h, g in same + [mate[1:]] * (halves - 1):
            i = h * gz_size + g

            @pl.when(i < mine if before else i > mine)
            def _():
                pl.semaphore_signal(sem, inc=1, device_id=(gx, h, g), device_id_type=MESH)

    greet(barrier, False)
    for load in depth_loads[1:]:
        load.start()
    load_place.start()
    below = lax.div(mine, halves) + part
    above = crowd // halves + halves - 2 - below

    @pl.when(gx + below > 0)
    def _():
        pl.semaphore_wait(barrier, gx * len(across) + below)

    greet(ready.at[gx], True)

    def contract(first, last):
        acc = jnp.zeros((points, coeffs.shape[1]), F32)
        for i in range(first, last):
            s, n = spans[i]
            depth_loads[i].wait()
            acc += dot(vals[:, s : s + n], coeffs[s : s + n, :], 1, 0)
        return acc

    load_core.wait()
    for a in range(gx_size):
        cores[a] = core[:, a * points : (a + 1) * points]
    for d in steps[::2]:

        @pl.when(gx >= d)
        def _():
            lend(gx - d)

    load_vals.wait()
    for d in steps[::2]:

        @pl.when(gx >= d)
        def _():
            row_win_copy(gx - d).start()

    occ = contract(0, len(spans))
    occ = occ.astype(BF16)
    col_occ[own] = occ
    @pl.when(above > 0)
    def _():
        pl.semaphore_wait(ready.at[gx], above)

    if halves > 1:
        col_fwd(gy).start()
    for h in sides:
        col_copy(h).start()
    square = jnp.square(occ.astype(F32))
    high = square.astype(BF16)
    low = (square - high.astype(F32)).astype(BF16)
    ones = jnp.ones((8, occ.shape[1]), BF16)
    dens[gx] = (dot(ones, high, 1, 1) + dot(ones, low, 1, 1))[:1]

    for t in range(gx_size - 1):

        @pl.when(gx > t)
        def _():
            dens_copy(t).start()

        @pl.when((gx > t) & (lax.rem(jnp.abs(gx - t), 2) == 1))
        def _():
            for k in range(halves):
                row_copy(t, k).start()

    for h in sides:
        col_win_copy(h).start()
    for h in range(gy_size):
        stage[h, :, :width] = vals[:, h * width : (h + 1) * width]
        if width < span:
            stage[h, :, width:] = jnp.zeros((points, span - width), BF16)
    lead = part == halves - 1

    @pl.when(lead)
    def _():
        for h in sides:
            cols_copy(h).start()

    own_cols = pltpu.make_async_copy(stage.at[gy], cols.at[gy], load_sem.at[3])
    own_cols.start()
    for t in range(1, gx_size):

        @pl.when(gx < t)
        def _():
            pl.semaphore_wait(ready.at[t], len(across))
            dens_copy(t).start()

        @pl.when((gx < t) & (lax.rem(jnp.abs(gx - t), 2) == 0))
        def _():
            lend(t)
            row_win_copy(t).start()
            for k in range(halves):
                row_copy(t, k).start()

    for h, g in same:
        pl.semaphore_signal(known, inc=1, device_id=(gx, h, g), device_id_type=MESH)
    col_win[gy] = vals[:, :lanes]
    load_place.wait()
    for z in range(gx_size):

        @pl.when(jnp.logical_not(keeps(z)))
        def _():
            row_win[z] = jnp.zeros(row_win.shape[1:], BF16)
            core_t[z] = jnp.zeros(core_t.shape[1:], BF16)

        @pl.when((gx != z) & jnp.logical_not(keeps(z)))
        def _():
            row_occ[pl.ds(z * halves, halves)] = jnp.zeros((halves, *row_occ.shape[1:]), BF16)

        @pl.when((gx != z) & jnp.logical_not(kept_by(z)))
        def _():
            tot_recv[pl.ds(z * crowd, crowd)] = jnp.zeros((crowd, *tot_recv.shape[1:]), BF16)

    spread = place[...]
    for k in range(halves):

        @pl.when(part == k)
        def _():
            starts = [a * points + k * half for a in range(gx_size)]
            core_q[...] = jnp.concatenate([core[:, s : s + half] for s in starts], axis=1)

    if sides:
        arrive(col_occ.at[pl.ds(0, len(sides))], col_sem)
    if halves > 1:
        for h in sides:
            col_fwd(h).start()
    if sides:
        arrive(col_win.at[pl.ds(0, len(sides))], col_win_sem)
    wins = dot(spread, col_win[...].reshape(side, lanes), 0, 1)
    win_t[...] = wins.reshape(win_t.shape)
    win_rows = wins.astype(BF16)

    if halves > 1:
        arrive(col_occ.at[pl.ds(0, gy_size)], col_sem, 1)
    for k in range(halves):
        row_occ[gx * halves + k] = col_occ[gy * halves + k, own_rows]
    tight = win_t.shape[1]
    layers = tight // 8

    if planes:
        arrive(dens.at[pl.ds(0, len(planes))], dens_sem)
    density = jnp.concatenate([dens[z] for z in range(gx_size)], axis=1)
    density = jnp.broadcast_to(density, (8, core.shape[1])).astype(BF16)
    potential = dot(density, core[...], 1, 1)[:1]
    pot_send[...] = potential
    if same:
        pl.semaphore_wait(known, len(same))
    for h, g in flat:
        pot_copy(h, g).start()

    def side_occ(k):
        return jnp.concatenate([col_occ[h * halves + k] for h in range(gy_size)], axis=0)

    def line_occ(k):
        return jnp.concatenate([row_occ[z * halves + k] for z in range(gx_size)], axis=0)

    for d in steps:
        z = other(d)

        @pl.when(inside(z))
        def _():
            lane_wait(row_win.at[z], row_win_sem, z)
            lane_wait(core_t.at[z], core_sem, z)

    far_win = dot(spread, row_win[...].reshape(-1, lanes), 0, 1).astype(BF16)

    for d in steps:
        z = other(d)

        @pl.when(inside(z))
        def _():
            lane_wait(row_occ.at[pl.ds(z * halves, halves)], row_sem, z)

    gram = sum(dot(side_occ(k), line_occ(k), 1, 1) for k in range(halves))
    mixed = (core_q[...].astype(F32) * gram).astype(BF16)
    block = dot(win_rows, mixed, 1, 0)
    bands = []
    for j in range(layers):
        starts = [g * tight + j * 8 for g in range(gz_size)]
        bands.append(jnp.concatenate([block[at : at + 8] for at in starts], axis=0))
    for z in reversed(range(gx_size)):
        pack = [band[:, z * half : (z + 1) * half] for band in bands]
        pack = jnp.concatenate(pack, axis=1).reshape(tot_send.shape[1:])
        tot_send[z] = pack.astype(BF16)

        @pl.when(keeps(z))
        def _():
            sweep(lambda i: tot_copy(z, *seat(i)).start())

    for h, g in flat:
        tot_copy(gx, h, g).start()
    own_tot = pltpu.make_async_copy(
        tot_send.at[gx, gz], tot_recv.at[gx * crowd + mine], tot_sem.at[1, gx]
    )
    own_tot.start()
    core_vals = [
        core_t[:, h].reshape(gx_size * half, points).astype(F32) for h in range(gy_size)
    ]
    gram = sum(dot(line_occ(k), side_occ(k), 1, 1) for k in range(halves))
    mixed = (jnp.concatenate(core_vals, axis=1) * gram).astype(BF16)
    back = dot(far_win, mixed, 1, 0)
    back_send[...] = back.reshape(back_send.shape).astype(BF16)
    for h, g in flat:
        back_copy(h, g).start()
    own_back = pltpu.make_async_copy(back_send.at[gz], back_recv.at[mine], back_sem.at[1])
    own_back.start()

    if sides:

        @pl.when(lead)
        def _():
            arrive(cols.at[pl.ds(0, len(sides))], cols_sem)
            if halves > 1:
                for h in sides:
                    cols_fwd(h).start()

    spare = 8 - rows
    reach = z_send.shape[3]
    tail = span - reach

    def spread_out(index, left):
        gap = jnp.zeros((spare, side), F32)
        lines = []
        for a in range(gx_size):
            lines += [left[a * rows : (a + 1) * rows], gap]
        lefts = jnp.concatenate(lines, axis=0).astype(BF16)
        out = dot(lefts, cols[...].reshape(side, span), 1, 0).reshape(gx_size, 8, span)
        line = lax.broadcasted_iota(jnp.int32, (8, tail), 0)
        for a in range(gx_size):
            for j in range(reach // tail):
                block = out[a, :, j * tail : (j + 1) * tail]
                if j * spare < rows:
                    moved = pltpu.roll(out[a, :, reach:], (rows - j * spare) % 8, 0)
                    block = jnp.where(line < rows, block, moved)
                z_send[index, a, :, j * tail : (j + 1) * tail] = block.astype(BF16)
            if reach % tail:
                at = reach // tail * tail
                z_send[index, a, :, at:] = out[a, :, at:reach].astype(BF16)
        for t in range(gx_size):

            @pl.when(gx != t)
            def _():
                z_copy(index, t).start()

    if flat:
        arrive(pot_recv.at[pl.ds(0, len(flat))], pot_sem)
    pot = pot_send[...]
    for h, g in flat:
        pot += pot_recv[h * gz_size + g]
    weighted = (win_t[gz] * pot).astype(BF16).astype(F32)
    own_cols.wait()
    if halves > 1 and sides:

        @pl.when(part == 0)
        def _():
            arrive(cols.at[pl.ds(0, len(sides))], cols_fwd_sem)

    spread_out(0, weighted)

    arrive(back_recv, back_sem)
    for z in range(gx_size):

        @pl.when((gx == z) | kept_by(z))
        def _():
            lane_wait(tot_recv.at[pl.ds(z * crowd, crowd)], tot_sem, z)

    total_of = []
    for i in range(gy_size * halves):
        h, k = divmod(i, halves)
        slots = [
            z * crowd + h * gz_size + g
            for z in range(gx_size)
            for g in range(k, gz_size, halves)
        ]
        total_of.append(sum(tot_recv[slot].astype(F32) for slot in slots))
    owned = [
        jnp.concatenate([one[:, j * half : (j + 1) * half] for one in total_of], axis=1)
        for j in range(layers)
    ]
    owned = jnp.concatenate(owned, axis=0)
    owned += sum(back_recv[i].astype(F32) for i in range(crowd)).reshape(owned.shape)
    spread_out(1, owned)

    if sides:
        leave(col_win.at[pl.ds(0, len(sides))], col_win_sem)

        @pl.when(lead)
        def _():
            leave(cols.at[pl.ds(0, len(sides))], cols_sem)
            if halves > 1:
                leave(cols.at[pl.ds(0, len(sides))], cols_fwd_sem)

    if planes:
        leave(dens.at[pl.ds(0, len(planes))], dens_sem)
    leave(col_occ.at[pl.ds(0, len(sides) + gy_size * (halves - 1))], col_sem)
    leave(pot_recv.at[pl.ds(0, len(flat))], pot_sem)
    leave(back_recv.at[pl.ds(0, len(flat))], back_sem)
    lane_leave(tot_recv.at[pl.ds(0, len(flat))], tot_sem, gx)
    for d in steps:
        t, z = keeper(d), other(d)

        @pl.when(inside(t))
        def _():
            lane_leave(row_occ.at[pl.ds(0, halves)], row_sem, t)
            lane_leave(row_win.at[0], row_win_sem, t)
            lane_leave(core_t.at[0], core_sem, t)

        @pl.when(inside(z))
        def _():
            lane_leave(tot_recv.at[pl.ds(0, crowd)], tot_sem, z)


    for index in range(2):
        if planes:
            arrive(z_recv.at[index, pl.ds(0, len(planes))], z_sem, index)
        acc = z_send[index, gx].astype(F32)
        for z in planes:
            acc += z_recv[index, z].astype(F32)
        out_ref[index, :, :reach] = acc[:rows]
        for r in range(rows):
            j, k = divmod(r, spare)
            line = acc[rows + k : rows + k + 1, j * tail : j * tail + width - reach]
            out_ref[index, r : r + 1, reach:] = line

    if planes:
        leave(z_recv.at[:, pl.ds(0, len(planes))], z_sem)


def local(colloc, occ_coeffs, core):
    points, total = colloc.shape
    gx_size = lax.axis_size("gx")
    gy_size = lax.axis_size("gy")
    gz_size = lax.axis_size("gz")
    occupied = occ_coeffs.shape[1]
    rows = W // (gx_size * gz_size)
    width = total // gy_size
    row_count, flat = core.shape[0], core.shape[2]
    lanes = up(W, LANES)
    side = gy_size * points
    span = up(width, LANES)
    halves = 2 if gz_size % 2 == 0 else 1
    half = points // halves
    tiles = span // LANES
    spare = 8 - rows
    tail = max(t for t in range(1, tiles) if (tiles - t) // t * spare >= rows)
    reach = span - tail * LANES

    used = gx_size * rows
    tight = up(used, 8)
    place = np.zeros((lanes, gz_size, tight), np.float32)
    for a in range(gx_size):
        for g in range(gz_size):
            for k in range(rows):
                place[(a * gz_size + g) * rows + k, g, a * rows + k] = 1
    place = jnp.asarray(place.reshape(lanes, gz_size * tight), BF16)

    dims = (gx_size, gy_size, gz_size, rows, width)
    dma = pltpu.SemaphoreType.DMA
    vmem = pltpu.VMEM
    result = pl.pallas_call(
        functools.partial(kernel, dims),
        out_shape=pltpu.VMEM((2, rows, width), F32),
        in_specs=[pl.BlockSpec(memory_space=pltpu.HBM)] * 4,
        out_specs=pl.BlockSpec(memory_space=pltpu.VMEM),
        scratch_shapes=[
            vmem((points, total), BF16),
            vmem((total, occupied), BF16),
            vmem((row_count, flat), BF16),
            vmem(place.shape, BF16),
            vmem((row_count, gx_size * half), BF16),
            vmem((gx_size, row_count, points), BF16),
            vmem((gx_size, gy_size, half, points), BF16),
            vmem((gx_size, half, lanes), BF16),
            vmem((gx_size * halves, half, occupied), BF16),
            vmem((gy_size * halves, points, occupied), BF16),
            vmem((gy_size, points, lanes), BF16),
            vmem((gz_size, tight, side), F32),
            vmem((gx_size, 1, points), F32),
            vmem((gy_size, points, span), BF16),
            vmem((gy_size, points, span), BF16),
            vmem((1, side), F32),
            vmem((gy_size * gz_size, 1, side), F32),
            vmem((gx_size, gz_size, 8, tight // 8 * half), BF16),
            vmem((gx_size * gy_size * gz_size, 8, tight // 8 * half), BF16),
            vmem((gz_size, tight // 8, 8, side), BF16),
            vmem((gy_size * gz_size, tight // 8, 8, side), BF16),
            vmem((2, gx_size, 8, reach), BF16),
            vmem((2, gx_size, 8, reach), BF16),
            dma((4,)),
            dma((-(-total // DEPTH),)),
            pltpu.SemaphoreType.REGULAR((gx_size,)),
            pltpu.SemaphoreType.REGULAR,
            dma((2, gx_size)),
            dma((2, gx_size)),
            dma((2, gx_size)),
            dma((3,)),
            dma((2,)),
            dma((2,)),
            dma((2,)),
            dma((2,)),
            dma((2,)),
            dma((2, gx_size)),
            dma((2,)),
            dma((3,)),
        ],
        compiler_params=pltpu.CompilerParams(
            collective_id=0, has_side_effects=True, vmem_limit_bytes=60 * 1024 * 1024
        ),
    )(colloc, occ_coeffs, core.reshape(row_count, flat), place)
    return result[0], result[1]


def solution(mesh):
    in_specs = (P(("gx", "gy"), None), P(None, "gz"), P("gx", "gy", None))
    out_specs = (P(("gx", "gz"), "gy"), P(("gx", "gz"), "gy"))
    return jax.shard_map(local, mesh=mesh, in_specs=in_specs, out_specs=out_specs, check_vma=False)
```
